32 devices in a mesh: dp: 4 (over y, z), tp: 8 (over x, core).
Axes of the slice: x: 4, y: 2, z: 2, core: 2. Of those that a mesh axis runs over, the one named last changes fastest.
The devices are a block of a 4x4x8 slice.
Arguments:
- token_ids: int32 [32768], P('dp'), parts along dimension 0
- positions: int32 [32768], P('dp'), parts along dimension 0
- embed_table: bfloat16 [257216, 2048], P('tp')
- norm_scale: float32 [2048], replicated
- w_query: bfloat16 [2048, 2048], P(None, 'tp')
- w_key: bfloat16 [2048, 256], replicated
- w_value: bfloat16 [2048, 256], replicated
Outputs:
- output 1: bfloat16 [32768, 2048], P(('dp', 'tp')), parts along dimension 0
- output 2: bfloat16 [32768, 8, 256], P('dp', 'tp'), parts along dimension 0
- output 3: bfloat16 [32768, 8, 256], P('dp', 'tp'), parts along dimension 0
- output 4: bfloat16 [32768, 8, 256], P('dp', 'tp'), parts along dimension 0
There are 4 independent parts. The reference program is written for one: setup_inputs(seed, part) draws one part's arguments, and reference() takes and returns one part's arrays. A program takes and returns all parts, laid end to end along the dimension named above; an argument that names none is the same for every part.
All inputs are finite; a program needn't handle non-finite values.
Results may differ from the reference program's by a relative error of at most 0.0120276.
Values are sent between devices in bfloat16 or wider.
A program may use at most 768 MiB of HBM per device.

```python
import math
import numpy as np
import jax
import jax.numpy as jnp
from jax import lax

D = 2048
HEADS = 8
KV_HEADS = 1
VOCAB = 257216
HEAD_DIM = 256
TOKENS = 8192
KV_SLOTS = 8
START_ODDS = 256
LEVELS = 16

ID_CAPS = np.minimum(VOCAB, 16 * 2 ** np.arange(LEVELS))


def draw_ids(key):
    level_key, id_key = jax.random.split(key)
    levels_drawn = jax.random.randint(level_key, (TOKENS,), 0, LEVELS)
    upper_ids = jnp.asarray(ID_CAPS, dtype=jnp.int32)[levels_drawn]
    token_ids = jax.random.randint(id_key, (TOKENS,), 0, upper_ids, dtype=jnp.int32)
    return token_ids.at[0].set(VOCAB - 1).at[1].set(0)


def draw_positions(key):
    step_ids = jnp.arange(TOKENS, dtype=jnp.int32)
    is_start = jax.random.randint(key, (TOKENS,), 0, START_ODDS, dtype=jnp.int32) == 0
    is_start = is_start.at[0].set(True)
    start_ids = lax.cummax(jnp.where(is_start, step_ids, 0), axis=0)
    return step_ids - start_ids


def setup_inputs(seed: int = 0, part: int = 0) -> dict:
    root_key = jax.random.key(seed)
    part_key = jax.random.fold_in(root_key, part)
    id_key, pos_key = jax.random.split(part_key)
    shared = jax.random.split(root_key, 6)
    row_scale = jax.random.uniform(shared[0], (VOCAB, 1), jnp.float32, 0.25, 2.0)
    embed_table = (jax.random.normal(shared[1], (VOCAB, D), jnp.float32) * (row_scale * D ** -0.5)).astype(jnp.bfloat16)
    norm_scale = 0.5 * jax.random.normal(shared[2], (D,), jnp.float32)
    w_query = (jax.random.normal(shared[3], (D, HEADS * HEAD_DIM), jnp.float32) * D ** -0.5).astype(jnp.bfloat16)
    w_key = (jax.random.normal(shared[4], (D, KV_HEADS * HEAD_DIM), jnp.float32) * D ** -0.5).astype(jnp.bfloat16)
    w_value = (jax.random.normal(shared[5], (D, KV_HEADS * HEAD_DIM), jnp.float32) * D ** -0.5).astype(jnp.bfloat16)
    return {"token_ids": draw_ids(id_key), "positions": draw_positions(pos_key), "embed_table": embed_table, "norm_scale": norm_scale, "w_query": w_query, "w_key": w_key, "w_value": w_value}


def rotate(head_vals, cosines, sines):
    half_dim = HEAD_DIM // 2
    front_half = head_vals[..., :half_dim]
    back_half = head_vals[..., half_dim:]
    return jnp.concatenate([front_half * cosines - back_half * sines, back_half * cosines + front_half * sines], axis=-1)


def reference(token_ids, positions, embed_table, norm_scale, w_query, w_key, w_value):
    normalizer = jnp.asarray(math.sqrt(D), dtype=jnp.bfloat16)
    residual = jnp.take(embed_table, token_ids, axis=0) * normalizer
    widened = residual.astype(jnp.float32)
    inv_rms = lax.rsqrt(jnp.mean(widened * widened, axis=-1, keepdims=True) + 1e-6)
    normed = (widened * inv_rms * (1.0 + norm_scale)).astype(jnp.bfloat16)
    inv_freq = 10000.0 ** (-jnp.arange(0, HEAD_DIM, 2, dtype=jnp.float32) / HEAD_DIM)
    angles = positions.astype(jnp.float32)[:, None] * inv_freq[None, :]
    cosines = jnp.cos(angles)[:, None, :]
    sines = jnp.sin(angles)[:, None, :]
    q_lin = jnp.dot(normed, w_query, preferred_element_type=jnp.float32).astype(jnp.bfloat16)
    k_lin = jnp.dot(normed, w_key, preferred_element_type=jnp.float32).astype(jnp.bfloat16)
    v_lin = jnp.dot(normed, w_value, preferred_element_type=jnp.float32).astype(jnp.bfloat16)
    queries = (rotate(q_lin.reshape(TOKENS, HEADS, HEAD_DIM).astype(jnp.float32), cosines, sines) * HEAD_DIM ** -0.5).astype(jnp.bfloat16)
    keys_rot = rotate(k_lin.reshape(TOKENS, KV_HEADS, HEAD_DIM).astype(jnp.float32), cosines, sines).astype(jnp.bfloat16)
    repeats = KV_SLOTS // KV_HEADS
    key_heads = jnp.repeat(keys_rot, repeats, axis=1)
    value_heads = jnp.repeat(v_lin.reshape(TOKENS, KV_HEADS, HEAD_DIM), repeats, axis=1)
    return (residual, queries, key_heads, value_heads)
```

```python
import functools
import math
import jax
import jax.numpy as jnp
import numpy as np
from jax import lax
from jax.experimental import pallas as pl
from jax.experimental.pallas import tpu as pltpu
from jax.sharding import PartitionSpec as P

HEAD_DIM = 256
EPSILON = 1e-6
ROPE_BASE = 10000.0
CHUNK = 64
PICK = 32
SLAB = 8
DEPTH = 4
CORES = 2
VMEM_LIMIT = 60 * 1024 * 1024


def rope_tables(positions):
    inv_freq = ROPE_BASE ** (-jnp.arange(0, HEAD_DIM, 2, dtype=jnp.float32) / HEAD_DIM)
    angles = positions.astype(jnp.float32)[:, None] * inv_freq[None, :]
    return jnp.cos(angles), jnp.sin(angles)


def rms_norm(resid_rows, norm_scale):
    widened = resid_rows.astype(jnp.float32)
    inv_rms = lax.rsqrt(jnp.mean(widened * widened, axis=-1, keepdims=True) + EPSILON)
    return (widened * inv_rms * (1.0 + norm_scale)).astype(jnp.bfloat16)


def rotate(head_vals, cosines, sines):
    half_dim = head_vals.shape[-1] // 2
    front_half = head_vals[..., :half_dim]
    back_half = head_vals[..., half_dim:]
    return jnp.concatenate([front_half * cosines - back_half * sines, back_half * cosines + front_half * sines], axis=-1)


def project(normed, weight, cosines, sines, factor):
    linear = jnp.dot(normed, weight, preferred_element_type=jnp.float32).astype(jnp.bfloat16)
    head_view = linear.reshape(linear.shape[0], -1, HEAD_DIM).astype(jnp.float32)
    return (rotate(head_view, cosines, sines) * factor).astype(jnp.bfloat16)


def dense_path(token_ids, positions, table_rows, norm_scale, w_query, key_cols, value_cols):
    dev_index = lax.axis_index("tp")
    vocab_rows, model_width = table_rows.shape
    normalizer = jnp.asarray(math.sqrt(model_width), dtype=jnp.bfloat16)
    local_ids = token_ids - dev_index * vocab_rows
    inside = (local_ids >= 0) & (local_ids < vocab_rows)
    picked = jnp.take(table_rows, local_ids, axis=0, mode="clip") * normalizer
    partial = jnp.where(inside[:, None], picked, jnp.zeros((), jnp.bfloat16))
    residual = lax.psum_scatter(partial, "tp", scatter_dimension=0, tiled=True)
    normed = lax.all_gather(rms_norm(residual, norm_scale), "tp", axis=0, tiled=True)
    cosines, sines = rope_tables(positions)
    cosines, sines = cosines[:, None, :], sines[:, None, :]
    queries = project(normed, w_query, cosines, sines, HEAD_DIM ** -0.5)
    key_heads = project(normed, key_cols, cosines, sines, 1.0)
    value_lin = jnp.dot(normed, value_cols, preferred_element_type=jnp.float32).astype(jnp.bfloat16)
    return residual, queries[:, 0, :], key_heads[:, 0, :], value_lin


class Plan:
    def __init__(self, group_size, tokens, vocab_rows):
        unit = CHUNK * 2
        self.hot = min(tokens // 8, vocab_rows // unit * unit)
        share = [11 / 32, 5 / 64] + [3 / 64] * 2
        room = [share[o] if o < 4 else 3 / 128 for o in range(group_size)]
        self.caps = [max(CHUNK, -(-int(tokens * r) // CHUNK) * CHUNK) for r in room]
        self.bases, at = [], self.hot
        for cap in self.caps:
            self.bases.append(at)
            at += cap
        self.rows = at
        self.list_rows = -(-(-(-max(self.caps) // 128)) // 8) * 8


def choose(values, index):
    out = jnp.int32(values[0])
    for j in range(1, len(values)):
        out = jnp.where(index == j, jnp.int32(values[j]), out)
    return out


def prep_kernel(plan, group_size, vocab_rows, ids_ref, slot_ref, list_ref, count_ref):
    me = lax.axis_index("tp")
    ids = ids_ref[...]
    blocks, lanes = ids.shape
    cold = ids >= plan.hot
    masks = [cold & (ids >= o * vocab_rows) & (ids < (o + 1) * vocab_rows) for o in range(group_size)]
    stack = jnp.concatenate([m.astype(jnp.float32) for m in masks], axis=0)
    stack = stack.astype(jnp.bfloat16)
    tri_r = lax.broadcasted_iota(jnp.int32, (lanes, lanes), 0)
    tri_c = lax.broadcasted_iota(jnp.int32, (lanes, lanes), 1)
    upper = (tri_r <= tri_c).astype(jnp.float32).astype(jnp.bfloat16)
    within = jnp.dot(stack, upper, preferred_element_type=jnp.float32)
    totals = jnp.dot(stack, jnp.ones((lanes, lanes), jnp.bfloat16), preferred_element_type=jnp.float32)
    low_r = lax.broadcasted_iota(jnp.int32, (blocks, blocks), 0)
    low_c = lax.broadcasted_iota(jnp.int32, (blocks, blocks), 1)
    lower = (low_c < low_r).astype(jnp.float32).astype(jnp.bfloat16)
    slot = jnp.where(cold, 0, ids)
    own_rank = jnp.full((blocks, lanes), -1, jnp.int32)
    for o in range(group_size):
        tot = totals[o * blocks:(o + 1) * blocks]
        before = jnp.dot(lower, tot.astype(jnp.bfloat16), preferred_element_type=jnp.float32)
        rank = (before + within[o * blocks:(o + 1) * blocks]).astype(jnp.int32) - 1
        slot = slot + jnp.where(masks[o], jnp.minimum(rank, plan.caps[o] - 1) + plan.bases[o], 0)
        own_rank = jnp.where(masks[o] & (me == o), rank, own_rank)
        count_ref[o:o + 1, :] = (before[blocks - 1:] + tot[blocks - 1:]).astype(jnp.int32)
    slot_ref[...] = slot
    local = jnp.where(own_rank >= 0, ids - me * vocab_rows, 0)
    major, minor = own_rank >> 7, own_rank & 127
    high, low = local >> 8, local & 255
    iota_major = lax.broadcasted_iota(jnp.int32, (plan.list_rows, lanes), 0)
    iota_minor = lax.broadcasted_iota(jnp.int32, (lanes, lanes), 0)
    acc = jnp.zeros((2 * plan.list_rows, lanes), jnp.float32)
    per = 8
    for g in range(blocks // per):
        lhs, rhs = [], []
        for r in range(g * per, (g + 1) * per):
            hit = iota_major == major[r:r + 1, :]
            lhs.append(jnp.concatenate([jnp.where(hit, high[r:r + 1, :], 0), jnp.where(hit, low[r:r + 1, :], 0)], axis=0).astype(jnp.float32))
            rhs.append((iota_minor == minor[r:r + 1, :]).astype(jnp.float32))
        left = jnp.concatenate(lhs, axis=1).astype(jnp.bfloat16)
        right = jnp.concatenate(rhs, axis=1).astype(jnp.bfloat16)
        acc = acc + lax.dot_general(left, right, (((1,), (1,)), ((), ())), preferred_element_type=jnp.float32)
    whole = acc.astype(jnp.int32)
    list_ref[...] = whole[:plan.list_rows] * 256 + whole[plan.list_rows:]


def prepare(plan, group_size, vocab_rows, token_ids):
    blocks = token_ids.shape[0] // 128
    return pl.pallas_call(
        functools.partial(prep_kernel, plan, group_size, vocab_rows),
        out_shape=(
            jax.ShapeDtypeStruct((blocks, 128), jnp.int32),
            jax.ShapeDtypeStruct((plan.list_rows, 128), jnp.int32),
            jax.ShapeDtypeStruct((group_size, 128), jnp.int32),
        ),
        compiler_params=pltpu.CompilerParams(vmem_limit_bytes=VMEM_LIMIT),
        name="slots",
    )(token_ids.reshape(blocks, 128))


def pick_rows(rows_smem, total, source, emit, slabs, onehot, sem):
    groups = (total + PICK - 1) // PICK

    def fetch(g):
        place = lax.rem(g, DEPTH)
        lane = lax.broadcasted_iota(jnp.int32, (1, PICK * SLAB), 1)
        for i in range(PICK):
            row = rows_smem[g * PICK + i]
            start = pl.multiple_of((row >> 3) << 3, SLAB)
            pltpu.make_async_copy(source.at[pl.ds(start, SLAB)], slabs.at[place, pl.ds(i * SLAB, SLAB)], sem.at[place]).start()
            onehot[place, pl.ds(i, 1), :] = jnp.where(lane == (row & 7) + i * SLAB, 1.0, 0.0)

    for g in range(DEPTH - 1):
        @pl.when(g < groups)
        def _():
            fetch(g)

    def body(g, carry):
        place = lax.rem(g, DEPTH)

        @pl.when(g + DEPTH - 1 < groups)
        def _():
            fetch(g + DEPTH - 1)

        pltpu.make_async_copy(source.at[pl.ds(0, PICK * SLAB)], slabs.at[place], sem.at[place]).wait()
        picked = jnp.dot(onehot[place].astype(jnp.bfloat16), slabs[place], preferred_element_type=jnp.float32)
        emit(g, picked)
        return carry

    lax.fori_loop(0, groups, body, 0)
    return groups


def gather_kernel(plan, normalizer, counts, rows_smem, table, out, slabs, onehot, stage, hot_in, sem, out_sem, hot_sem):
    me = lax.axis_index("tp")
    total = jnp.minimum(counts[me], choose(plan.caps, me))
    base = choose(plan.bases, me)
    scale = jnp.float32(normalizer)

    def emit(g, picked):
        side = lax.rem(g, 2)

        @pl.when(g >= 2)
        def _():
            pltpu.make_async_copy(stage.at[side], out.at[pl.ds(0, PICK)], out_sem.at[side]).wait()

        stage[side] = (picked * scale).astype(jnp.bfloat16)
        at = pl.multiple_of(base + g * PICK, PICK)
        pltpu.make_async_copy(stage.at[side], out.at[pl.ds(at, PICK)], out_sem.at[side]).start()

    @pl.when(me == 0)
    def _():
        step = hot_in.shape[1]
        n_steps = plan.hot // step
        def load(i):
            return pltpu.make_async_copy(table.at[pl.ds(i * step, step)], hot_in.at[i % 2], hot_sem.at[i % 2])
        def save(i):
            return pltpu.make_async_copy(hot_in.at[i % 2], out.at[pl.ds(i * step, step)], hot_sem.at[2 + i % 2])
        load(0).start()
        for i in range(n_steps):
            if i + 1 < n_steps:
                if i >= 1:
                    save(i - 1).wait()
                load(i + 1).start()
            load(i).wait()
            hot_in[i % 2] = (hot_in[i % 2].astype(jnp.float32) * scale).astype(jnp.bfloat16)
            save(i).start()
        if n_steps > 1:
            save(n_steps - 2).wait()
        save(n_steps - 1).wait()

    groups = pick_rows(rows_smem, total, table, emit, slabs, onehot, sem)
    for last in (2, 1):
        @pl.when(groups >= last)
        def _():
            side = lax.rem(groups - last, 2)
            pltpu.make_async_copy(stage.at[side], out.at[pl.ds(0, PICK)], out_sem.at[side]).wait()


def gather_rows(plan, normalizer, counts, rows, table):
    width = table.shape[1]
    hot_step = min(256, plan.hot)
    return pl.pallas_call(
        functools.partial(gather_kernel, plan, normalizer),
        out_shape=jax.ShapeDtypeStruct((plan.rows, width), table.dtype),
        in_specs=[pl.BlockSpec(memory_space=pltpu.SMEM), pl.BlockSpec(memory_space=pltpu.SMEM), pl.BlockSpec(memory_space=pl.ANY)],
        out_specs=pl.BlockSpec(memory_space=pl.ANY),
        scratch_shapes=[
            pltpu.VMEM((DEPTH, PICK * SLAB, width), table.dtype),
            pltpu.VMEM((DEPTH, PICK, PICK * SLAB), jnp.float32),
            pltpu.VMEM((2, PICK, width), table.dtype),
            pltpu.VMEM((2, hot_step, width), table.dtype),
            pltpu.SemaphoreType.DMA((DEPTH,)),
            pltpu.SemaphoreType.DMA((2,)),
            pltpu.SemaphoreType.DMA((4,)),
        ],
        compiler_params=pltpu.CompilerParams(vmem_limit_bytes=VMEM_LIMIT),
        cost_estimate=pl.CostEstimate(flops=2 * 2048 * 256 * 2816, bytes_accessed=100_000_000, transcendentals=0),
        name="owner_rows",
    )(counts, rows, table)


def resid_kernel(rows_smem, source, out, slabs, onehot, sem, *, count):
    def emit(g, picked):
        at = pl.multiple_of(g * PICK, PICK)
        out[pl.ds(at, PICK), :] = picked.astype(out.dtype)
    pick_rows(rows_smem, count, source, emit, slabs, onehot, sem)


def own_rows(source, rows):
    width, count = source.shape[1], rows.shape[0]
    return pl.pallas_call(
        functools.partial(resid_kernel, count=count),
        out_shape=jax.ShapeDtypeStruct((count, width), source.dtype),
        in_specs=[pl.BlockSpec(memory_space=pltpu.SMEM), pl.BlockSpec(memory_space=pl.ANY)],
        out_specs=pl.BlockSpec(memory_space=pltpu.VMEM),
        scratch_shapes=[
            pltpu.VMEM((DEPTH, PICK * SLAB, width), source.dtype),
            pltpu.VMEM((DEPTH, PICK, PICK * SLAB), jnp.float32),
            pltpu.SemaphoreType.DMA((DEPTH,)),
        ],
        compiler_params=pltpu.CompilerParams(vmem_limit_bytes=VMEM_LIMIT),
        name="own_residual",
    )(rows, source)


def multicast_kernel(plan, group_size, buf_in, buf, got, ring_sem, pair_sem):
    del buf_in
    chips = group_size // CORES
    me = lax.axis_index("tp")
    chip, core = lax.div(me, CORES), lax.rem(me, CORES)
    mate = chip * CORES + (1 - core)
    step = 1 - 2 * core

    def chip_at(delta):
        return lax.rem(chip + delta * step + 2 * chips, chips)

    ahead, behind = chip_at(1) * CORES + core, chip_at(-1) * CORES + core

    barrier = pltpu.get_barrier_semaphore()
    for other in (mate, ahead, behind):
        pl.semaphore_signal(barrier, inc=1, device_id={"tp": other}, device_id_type=pl.DeviceIdType.MESH)
    pl.semaphore_wait(barrier, 3)

    own_n = [c // CHUNK for c in plan.caps]
    own_n[0] += plan.hot // CHUNK
    own_at, at = [], 0
    for c in own_n:
        own_at.append(at)
        at += c
    first = [own_at[2 * c] for c in range(chips)]
    half = [(own_n[2 * c] + own_n[2 * c + 1]) // 2 for c in range(chips)]
    turn = [own_n[2 * c] - half[c] for c in range(chips)]

    def rows(j):
        return pl.ds(pl.multiple_of(j * CHUNK, CHUNK), CHUNK)

    def ring(j):
        return pltpu.make_async_remote_copy(src_ref=buf.at[rows(j)], dst_ref=buf.at[rows(j)], send_sem=ring_sem.at[j], recv_sem=got.at[j], device_id={"tp": ahead}, device_id_type=pl.DeviceIdType.MESH)

    def pair(j):
        return pltpu.make_async_remote_copy(src_ref=buf.at[rows(j)], dst_ref=buf.at[rows(j)], send_sem=pair_sem.at[j], recv_sem=got.at[j], device_id={"tp": mate}, device_id_type=pl.DeviceIdType.MESH)

    def loop(count, fn):
        def body(t, c):
            fn(t)
            return c
        lax.fori_loop(0, count, body, 0)

    my_first, my_half, my_turn = choose(first, chip), choose(half, chip), choose(turn, chip)
    mine = jnp.where(core == 0, my_half, my_half - my_turn)
    mine_at = jnp.where(core == 0, my_first, my_first + my_half + my_turn)
    cross_at = my_first + my_half

    @pl.when(core == 0)
    def _():
        loop(my_turn, lambda t: pair(cross_at + t).start())

    loop(mine, lambda t: ring(mine_at + t).start())
    loop(mine, lambda t: pair(mine_at + t).start())

    @pl.when(core == 1)
    def _():
        def relay(t):
            pair(cross_at + t).wait_recv()
            ring(cross_at + t).start()
        loop(my_turn, relay)

    for hop in range(1, chips):
        origin = chip_at(-hop)
        count = choose(half, origin)
        base = choose(first, origin) + core * count
        shift = core * choose(turn, origin)

        def arrive(t):
            j = base + lax.rem(t + shift, count)
            ring(j).wait_recv()
            if hop < chips - 1:
                ring(j).start()
            pair(j).start()
        loop(count, arrive)

    for hop in range(1, chips):
        origin = lax.rem(chip - hop * step + 2 * chips, chips)
        count = choose(half, origin)
        base = choose(first, origin) + (1 - core) * count
        loop(count, lambda t: pair(base + t).wait_recv())
    theirs = jnp.where(core == 0, my_half - my_turn, my_half)
    theirs_at = jnp.where(core == 0, my_first + my_half + my_turn, my_first)
    loop(theirs, lambda t: pair(theirs_at + t).wait_recv())

    @pl.when(core == 0)
    def _():
        loop(my_turn, lambda t: pair(cross_at + t).wait_send())

    @pl.when(core == 1)
    def _():
        loop(my_turn, lambda t: ring(cross_at + t).wait_send())

    def sent(t):
        ring(mine_at + t).wait_send()
        pair(mine_at + t).wait_send()
    loop(mine, sent)
    for hop in range(1, chips):
        origin = chip_at(-hop)
        count = choose(half, origin)
        base = choose(first, origin) + core * count

        def left(t):
            if hop < chips - 1:
                ring(base + t).wait_send()
            pair(base + t).wait_send()
        loop(count, left)


def multicast(plan, group_size, buf):
    chunks = plan.rows // CHUNK
    return pl.pallas_call(
        functools.partial(multicast_kernel, plan, group_size),
        out_shape=jax.ShapeDtypeStruct(buf.shape, buf.dtype),
        in_specs=[pl.BlockSpec(memory_space=pl.ANY)],
        out_specs=pl.BlockSpec(memory_space=pl.ANY),
        scratch_shapes=[pltpu.SemaphoreType.DMA((chunks,)), pltpu.SemaphoreType.DMA((chunks,)), pltpu.SemaphoreType.DMA((chunks,))],
        input_output_aliases={0: 0},
        compiler_params=pltpu.CompilerParams(collective_id=0, has_side_effects=True, vmem_limit_bytes=VMEM_LIMIT),
        cost_estimate=pl.CostEstimate(flops=100_000_000_000, bytes_accessed=100_000_000, transcendentals=0),
        name="multicast",
    )(buf)


def lin_kernel(rows_ref, scale_ref, wq_ref, wk_ref, wv_ref, out_ref):
    normed = rms_norm(rows_ref[...], scale_ref[...])
    n = rows_ref.shape[0]
    at = 0
    for w in (wq_ref, wk_ref, wv_ref):
        y = jnp.dot(normed, w[...], preferred_element_type=jnp.float32).astype(jnp.bfloat16).astype(jnp.float32)
        for j in range(y.shape[1] // 128):
            out_ref[pl.ds(at, n, stride=8), :] = y[:, j * 128:(j + 1) * 128]
            at += 1


def projections(buf, norm_scale, w_query, key_cols, value_cols):
    n, width = buf.shape
    block = 256 if n % 256 == 0 else CHUNK
    full = lambda i: (0, 0)
    return pl.pallas_call(
        lin_kernel,
        grid=(n // block,),
        out_shape=jax.ShapeDtypeStruct((n * 8, 128), jnp.float32),
        in_specs=[
            pl.BlockSpec((block, width), lambda i: (i, 0)),
            pl.BlockSpec((1, width), full),
            pl.BlockSpec(w_query.shape, full),
            pl.BlockSpec(key_cols.shape, full),
            pl.BlockSpec(value_cols.shape, full),
        ],
        out_specs=pl.BlockSpec((block * 8, 128), lambda i: (i, 0)),
        compiler_params=pltpu.CompilerParams(vmem_limit_bytes=VMEM_LIMIT),
        name="projections",
    )(buf, norm_scale.reshape(1, width), w_query, key_cols, value_cols)


TOK = 256


def expand_kernel(slots, lin, cos_ref, sin_ref, q_ref, k_ref, v_ref, store, spread, sem):
    step = pl.program_id(0)

    @pl.when(step == 0)
    def _():
        whole = pltpu.make_async_copy(lin, store, sem)
        whole.start()
        whole.wait()

    def body(b, carry):
        for i in range(32):
            t = b * 32 + i
            at = pl.multiple_of(slots[step * TOK + t], 8)
            spread[pl.ds(pl.multiple_of(t * 8, 8), 8), :] = store[pl.ds(at, 8), :]
        return carry

    lax.fori_loop(0, TOK // 32, body, 0)
    cosines, sines = cos_ref[...], sin_ref[...]
    parts = [spread[pl.ds(j, TOK, stride=8), :] for j in range(6)]
    factor = HEAD_DIM ** -0.5
    half = HEAD_DIM // 2
    q_ref[:, :half] = ((parts[0] * cosines - parts[1] * sines) * factor).astype(q_ref.dtype)
    q_ref[:, half:] = ((parts[1] * cosines + parts[0] * sines) * factor).astype(q_ref.dtype)
    k_ref[:, :half] = (parts[2] * cosines - parts[3] * sines).astype(k_ref.dtype)
    k_ref[:, half:] = (parts[3] * cosines + parts[2] * sines).astype(k_ref.dtype)
    v_ref[:, :half] = parts[4].astype(v_ref.dtype)
    v_ref[:, half:] = parts[5].astype(v_ref.dtype)


def expand(lin, slots, cosines, sines):
    tokens = slots.shape[0]
    head = jax.ShapeDtypeStruct((tokens, HEAD_DIM), jnp.bfloat16)
    out_spec = pl.BlockSpec((TOK, HEAD_DIM), lambda i, s: (i, 0))
    return pl.pallas_call(
        expand_kernel,
        grid_spec=pltpu.PrefetchScalarGridSpec(
            num_scalar_prefetch=1,
            grid=(tokens // TOK,),
            in_specs=[
                pl.BlockSpec(memory_space=pl.ANY),
                pl.BlockSpec((TOK, HEAD_DIM // 2), lambda i, s: (i, 0)),
                pl.BlockSpec((TOK, HEAD_DIM // 2), lambda i, s: (i, 0)),
            ],
            out_specs=[out_spec] * 3,
            scratch_shapes=[pltpu.VMEM(lin.shape, lin.dtype), pltpu.VMEM((TOK * 8, 128), jnp.float32), pltpu.SemaphoreType.DMA],
        ),
        out_shape=(head,) * 3,
        compiler_params=pltpu.CompilerParams(vmem_limit_bytes=VMEM_LIMIT),
        name="expand",
    )(slots * 8, lin, cosines, sines)


def solution(mesh):
    group_size = mesh.shape["tp"]

    def local_step(token_ids, positions, table_rows, norm_scale, w_query, w_key, w_value):
        dev_index = lax.axis_index("tp")
        vocab_rows, model_width = table_rows.shape
        tokens = token_ids.shape[0]
        normalizer = float(np.asarray(math.sqrt(model_width), dtype=jnp.bfloat16))
        kv_heads = w_key.shape[1] // HEAD_DIM
        slot_count = max(kv_heads, group_size)
        slots_here = slot_count // group_size
        first_head = (dev_index * slots_here) // (slot_count // kv_heads)
        if kv_heads * HEAD_DIM == slots_here * HEAD_DIM:
            key_cols, value_cols = w_key, w_value
        else:
            key_cols = lax.dynamic_slice_in_dim(w_key, first_head * HEAD_DIM, slots_here * HEAD_DIM, axis=1)
            value_cols = lax.dynamic_slice_in_dim(w_value, first_head * HEAD_DIM, slots_here * HEAD_DIM, axis=1)

        plan = Plan(group_size, tokens, vocab_rows)
        slots, rows, counts = prepare(plan, group_size, vocab_rows, token_ids)
        slots, rows, counts = slots.reshape(tokens), rows.reshape(-1), counts[:, 0]
        fits = jnp.all(counts <= jnp.asarray(plan.caps, jnp.int32))
        buf = gather_rows(plan, normalizer, counts, rows, table_rows)
        buf = multicast(plan, group_size, buf)

        def fast(buf):
            mine = tokens // group_size
            own = lax.dynamic_slice_in_dim(slots, dev_index * mine, mine)
            residual = own_rows(buf, own)
            lin = projections(buf, norm_scale, w_query, key_cols, value_cols)
            cosines, sines = rope_tables(positions)
            return (residual, *expand(lin, slots, cosines, sines))

        def slow(buf):
            return dense_path(token_ids, positions, table_rows, norm_scale, w_query, key_cols, value_cols)

        residual, queries, key_heads, value_heads = lax.cond(fits, fast, slow, buf)
        return residual, queries[:, None, :], key_heads[:, None, :], value_heads[:, None, :]

    head_spec = P("dp", "tp", None)
    return jax.shard_map(local_step, mesh=mesh, in_specs=(P("dp"), P("dp"), P("tp", None), P(), P(None, "tp"), P(), P()), out_specs=(P(("dp", "tp"), None), head_spec, head_spec, head_spec), check_vma=False)
```

```python
import functools
import math
import jax
import jax.numpy as jnp
import numpy as np
from jax import lax
from jax.experimental import pallas as pl
from jax.experimental.pallas import tpu as pltpu
from jax.sharding import PartitionSpec as P

HEAD_DIM = 256
EPSILON = 1e-6
ROPE_BASE = 10000.0
CHUNK = 64
PICK = 64
SLAB = 8
DEPTH = 4
CORES = 2
VMEM_LIMIT = 60 * 1024 * 1024


def inverse_freq():
    return ROPE_BASE ** (-jnp.arange(0, HEAD_DIM, 2, dtype=jnp.float32) / HEAD_DIM)


def rope_tables(positions):
    angles = positions.astype(jnp.float32)[:, None] * inverse_freq()[None, :]
    return jnp.cos(angles), jnp.sin(angles)


def rms_norm(resid_rows, norm_scale):
    widened = resid_rows.astype(jnp.float32)
    inv_rms = lax.rsqrt(jnp.mean(widened * widened, axis=-1, keepdims=True) + EPSILON)
    return (widened * inv_rms * (1.0 + norm_scale)).astype(jnp.bfloat16)


def rotate(head_vals, cosines, sines):
    half_dim = head_vals.shape[-1] // 2
    front_half = head_vals[..., :half_dim]
    back_half = head_vals[..., half_dim:]
    return jnp.concatenate([front_half * cosines - back_half * sines, back_half * cosines + front_half * sines], axis=-1)


def project(normed, weight, cosines, sines, factor):
    linear = jnp.dot(normed, weight, preferred_element_type=jnp.float32).astype(jnp.bfloat16)
    head_view = linear.reshape(linear.shape[0], -1, HEAD_DIM).astype(jnp.float32)
    return (rotate(head_view, cosines, sines) * factor).astype(jnp.bfloat16)


def dense_path(group_size, token_ids, positions, table_rows, norm_scale, w_query, key_cols, value_cols):
    dev_index = lax.axis_index("tp")
    vocab_rows, model_width = table_rows.shape
    normalizer = jnp.asarray(math.sqrt(model_width), dtype=jnp.bfloat16)
    local_ids = token_ids - dev_index * vocab_rows
    inside = (local_ids >= 0) & (local_ids < vocab_rows)
    picked = jnp.take(table_rows, local_ids, axis=0, mode="clip") * normalizer
    partial = jnp.where(inside[:, None], picked, jnp.zeros((), jnp.bfloat16))
    by_owner = partial.reshape(group_size, -1, model_width)
    residual = jnp.sum(lax.all_to_all(by_owner, "tp", 0, 0), axis=0)
    normed = rms_norm(residual, norm_scale)
    copies = jnp.broadcast_to(normed[None], (group_size, *normed.shape))
    normed = lax.all_to_all(copies, "tp", 0, 0).reshape(-1, model_width)
    cosines, sines = rope_tables(positions)
    cosines, sines = cosines[:, None, :], sines[:, None, :]
    queries = project(normed, w_query, cosines, sines, HEAD_DIM ** -0.5)
    key_heads = project(normed, key_cols, cosines, sines, 1.0)
    value_lin = jnp.dot(normed, value_cols, preferred_element_type=jnp.float32).astype(jnp.bfloat16)
    return residual, queries[:, 0, :], key_heads[:, 0, :], value_lin


class Plan:
    def __init__(self, group_size, tokens, vocab_rows):
        unit = CHUNK * 2
        self.hot = min(tokens // 8, vocab_rows // unit * unit)
        share = [11 / 32, 5 / 64] + [3 / 64] * 2
        room = [share[o] if o < 4 else 3 / 128 for o in range(group_size)]
        self.caps = [max(CHUNK, -(-int(tokens * r) // CHUNK) * CHUNK) for r in room]
        self.bases, at = [], self.hot
        for cap in self.caps:
            self.bases.append(at)
            at += cap
        self.rows = at
        self.list_rows = -(-(-(-max(self.caps) // 128)) // 8) * 8


def choose(values, index):
    out = jnp.int32(values[0])
    for j in range(1, len(values)):
        out = jnp.where(index == j, jnp.int32(values[j]), out)
    return out


def offsets_by_column(rows):
    offsets = (rows & (SLAB - 1)).astype(jnp.float32)
    fill = jnp.zeros((128 - rows.shape[0], 128), jnp.float32)
    return jnp.concatenate([offsets, fill], axis=0).T


def prep_kernel(plan, group_size, vocab_rows, ids_ref, slot_ref, list_ref, count_ref, offset_ref):
    me = lax.axis_index("tp")
    ids = ids_ref[...]
    blocks, lanes = ids.shape
    cold = ids >= plan.hot
    masks = [cold & (ids >= o * vocab_rows) & (ids < (o + 1) * vocab_rows) for o in range(group_size)]
    stack = jnp.concatenate([m.astype(jnp.float32) for m in masks], axis=0)
    stack = stack.astype(jnp.bfloat16)
    tri_r = lax.broadcasted_iota(jnp.int32, (lanes, lanes), 0)
    tri_c = lax.broadcasted_iota(jnp.int32, (lanes, lanes), 1)
    upper = (tri_r <= tri_c).astype(jnp.float32).astype(jnp.bfloat16)
    within = jnp.dot(stack, upper, preferred_element_type=jnp.float32)
    totals = jnp.dot(stack, jnp.ones((lanes, lanes), jnp.bfloat16), preferred_element_type=jnp.float32)
    low_r = lax.broadcasted_iota(jnp.int32, (blocks, blocks), 0)
    low_c = lax.broadcasted_iota(jnp.int32, (blocks, blocks), 1)
    lower = (low_c < low_r).astype(jnp.float32).astype(jnp.bfloat16)
    slot = jnp.where(cold, 0, ids)
    own_rank = jnp.full((blocks, lanes), -1, jnp.int32)
    over = jnp.zeros((1, lanes), jnp.int32)
    for o in range(group_size):
        tot = totals[o * blocks:(o + 1) * blocks]
        before = jnp.dot(lower, tot.astype(jnp.bfloat16), preferred_element_type=jnp.float32)
        rank = (before + within[o * blocks:(o + 1) * blocks]).astype(jnp.int32) - 1
        slot = slot + jnp.where(masks[o], jnp.minimum(rank, plan.caps[o] - 1) + plan.bases[o], 0)
        own_rank = jnp.where(masks[o] & (me == o), rank, own_rank)
        count = (before[blocks - 1:] + tot[blocks - 1:]).astype(jnp.int32)
        count_ref[o:o + 1, :] = count
        over = jnp.maximum(over, count - plan.caps[o])
    slot_ref[...] = slot
    count_ref[group_size:group_size + 1, :] = over
    local = jnp.where(own_rank >= 0, ids - me * vocab_rows, 0)
    major, minor = own_rank >> 7, own_rank & 127
    high, low = local >> 8, local & 255
    iota_major = lax.broadcasted_iota(jnp.int32, (plan.list_rows, lanes), 0)
    iota_minor = lax.broadcasted_iota(jnp.int32, (lanes, lanes), 0)
    acc = jnp.zeros((2 * plan.list_rows, lanes), jnp.float32)
    per = 8
    for g in range(blocks // per):
        lhs, rhs = [], []
        for r in range(g * per, (g + 1) * per):
            hit = iota_major == major[r:r + 1, :]
            lhs.append(jnp.concatenate([jnp.where(hit, high[r:r + 1, :], 0), jnp.where(hit, low[r:r + 1, :], 0)], axis=0).astype(jnp.float32))
            rhs.append((iota_minor == minor[r:r + 1, :]).astype(jnp.float32))
        left = jnp.concatenate(lhs, axis=1).astype(jnp.bfloat16)
        right = jnp.concatenate(rhs, axis=1).astype(jnp.bfloat16)
        acc = acc + lax.dot_general(left, right, (((1,), (1,)), ((), ())), preferred_element_type=jnp.float32)
    whole = acc.astype(jnp.int32)
    wanted = whole[:plan.list_rows] * 256 + whole[plan.list_rows:]
    list_ref[...] = wanted
    offset_ref[...] = offsets_by_column(wanted)


def prepare(plan, group_size, vocab_rows, token_ids):
    blocks = token_ids.shape[0] // 128
    return pl.pallas_call(
        functools.partial(prep_kernel, plan, group_size, vocab_rows),
        out_shape=(
            jax.ShapeDtypeStruct((blocks, 128), jnp.int32),
            jax.ShapeDtypeStruct((plan.list_rows, 128), jnp.int32),
            jax.ShapeDtypeStruct((group_size + 8, 128), jnp.int32),
            jax.ShapeDtypeStruct((128, 128), jnp.float32),
        ),
        compiler_params=pltpu.CompilerParams(vmem_limit_bytes=VMEM_LIMIT),
        name="slots",
    )(token_ids.reshape(blocks, 128))


class Picker:
    def __init__(self, rows_smem, begin, groups, offsets, source, slabs, sem):
        self.rows_smem, self.begin, self.groups = rows_smem, begin, groups
        self.offsets, self.source, self.slabs, self.sem = offsets, source, slabs, sem

    def fetch(self, g):
        place = lax.rem(jnp.int32(g), DEPTH)
        first = self.begin + jnp.minimum(g, jnp.maximum(self.groups - 1, 0)) * PICK
        for i in range(PICK):
            row = self.rows_smem[first + i]
            start = pl.multiple_of((row >> 3) << 3, SLAB)
            pltpu.make_async_copy(self.source.at[pl.ds(start, SLAB)], self.slabs.at[place, pl.ds(i * SLAB, SLAB)], self.sem.at[place]).start()

    def wait(self, g):
        place = lax.rem(jnp.int32(g), DEPTH)
        pltpu.make_async_copy(self.source.at[pl.ds(0, PICK * SLAB)], self.slabs.at[place], self.sem.at[place]).wait()

    def pick(self, g):
        place = lax.rem(jnp.int32(g), DEPTH)
        per = 128 // PICK
        block = self.offsets[pl.ds(pl.multiple_of(lax.rem(g, per) * PICK, PICK), PICK), :]
        lane = lax.broadcasted_iota(jnp.int32, (PICK, 128), 1)
        column = jnp.sum(jnp.where(lane == lax.div(g, per), block, 0.0), axis=1, keepdims=True).astype(jnp.int32)
        shape = (PICK, PICK * SLAB)
        hit = lax.broadcasted_iota(jnp.int32, shape, 1) == lax.broadcasted_iota(jnp.int32, shape, 0) * SLAB + column
        onehot = jnp.where(hit, 1.0, 0.0).astype(jnp.bfloat16)
        return jnp.dot(onehot, self.slabs[place], preferred_element_type=jnp.float32)

    def lead(self):
        for g in range(DEPTH - 1):
            self.fetch(g)

    def turn(self, g):
        self.wait(g)
        self.fetch(g + DEPTH - 1)
        return self.pick(g)

    def drain(self, groups):
        for g in range(DEPTH - 1):
            self.wait(groups + g)


def gather_kernel(plan, normalizer, counts, rows_smem, offsets, table, out, slabs, stage, hot_in, hot_out, sem, out_sem, hot_sem):
    me = lax.axis_index("tp")
    total = jnp.minimum(counts[me, 0], choose(plan.caps, me))
    base = choose(plan.bases, me)
    scale = jnp.float32(normalizer)
    groups = (total + PICK - 1) // PICK
    picker = Picker(rows_smem, 0, groups, offsets, table, slabs, sem)
    picker.lead()

    def emit(g, picked):
        side = lax.rem(g, 2)

        @pl.when(g >= 2)
        def _():
            pltpu.make_async_copy(stage.at[side], out.at[pl.ds(0, PICK)], out_sem.at[side]).wait()

        stage[side] = (picked * scale).astype(jnp.bfloat16)
        at = pl.multiple_of(base + g * PICK, PICK)
        pltpu.make_async_copy(stage.at[side], out.at[pl.ds(at, PICK)], out_sem.at[side]).start()

    step = hot_in.shape[1]
    hot_steps = jnp.where(me == 0, plan.hot // step, 0)

    def load(i):
        return pltpu.make_async_copy(table.at[pl.ds(pl.multiple_of(i * step, step), step)], hot_in.at[lax.rem(i, 2)], hot_sem.at[lax.rem(i, 2)])

    def save(i):
        return pltpu.make_async_copy(hot_out.at[lax.rem(i, 2)], out.at[pl.ds(pl.multiple_of(i * step, step), step)], hot_sem.at[2 + lax.rem(i, 2)])

    def hot_turn(i):
        @pl.when(i < hot_steps)
        def _():
            load(i).wait()

            @pl.when(i >= 2)
            def _():
                save(i - 2).wait()
            hot_out[lax.rem(i, 2)] = (hot_in[lax.rem(i, 2)].astype(jnp.float32) * scale).astype(jnp.bfloat16)
            save(i).start()

            @pl.when(i + 2 < hot_steps)
            def _():
                load(i + 2).start()

    for i in range(2):
        @pl.when(i < hot_steps)
        def _():
            load(jnp.int32(i)).start()

    def rest(i, carry):
        hot_turn(i)
        return carry

    def body(g, carry):
        emit(g, picker.turn(g))
        hot_turn(g)
        return carry

    lax.fori_loop(0, groups, body, 0)
    lax.fori_loop(groups, jnp.maximum(hot_steps, groups), rest, 0)
    picker.drain(groups)
    for back in (2, 1):
        @pl.when(hot_steps >= back)
        def _():
            save(hot_steps - back).wait()
    for last in (2, 1):
        @pl.when(groups >= last)
        def _():
            side = lax.rem(groups - last, 2)
            pltpu.make_async_copy(stage.at[side], out.at[pl.ds(0, PICK)], out_sem.at[side]).wait()


def gather_rows(plan, normalizer, counts, rows, offsets, table):
    width = table.shape[1]
    hot_step = CHUNK
    return pl.pallas_call(
        functools.partial(gather_kernel, plan, normalizer),
        out_shape=jax.ShapeDtypeStruct((plan.rows, width), table.dtype),
        in_specs=[pl.BlockSpec(memory_space=pltpu.SMEM), pl.BlockSpec(memory_space=pltpu.SMEM), pl.BlockSpec(memory_space=pltpu.VMEM), pl.BlockSpec(memory_space=pl.ANY)],
        out_specs=pl.BlockSpec(memory_space=pl.ANY),
        scratch_shapes=[
            pltpu.VMEM((DEPTH, PICK * SLAB, width), table.dtype),
            pltpu.VMEM((2, PICK, width), table.dtype),
            pltpu.VMEM((2, hot_step, width), table.dtype),
            pltpu.VMEM((2, hot_step, width), table.dtype),
            pltpu.SemaphoreType.DMA((DEPTH,)),
            pltpu.SemaphoreType.DMA((2,)),
            pltpu.SemaphoreType.DMA((4,)),
        ],
        compiler_params=pltpu.CompilerParams(vmem_limit_bytes=VMEM_LIMIT),
        cost_estimate=pl.CostEstimate(flops=2 * 2048 * 256 * 2816, bytes_accessed=100_000_000, transcendentals=0),
        name="owner_rows",
    )(counts, rows, offsets, table)


TOK = 512
TURN = 256
LAG = 2
HALF_PI = (1.5703125, 4.837512969970703e-4, 7.549789948768648e-8)
SIN_POLY = (-1.6666654611e-1, 8.3321608736e-3, -1.9515295891e-4)
COS_POLY = (4.166664568298827e-2, -1.388731625493765e-3, 2.443315711809948e-5)


def cos_sin(angles):
    turns = jnp.floor(angles * (2 / math.pi) + 0.5)
    x = angles - turns * HALF_PI[0]
    x = x - turns * HALF_PI[1]
    x = x - turns * HALF_PI[2]
    x2 = x * x
    sine = x + x * x2 * (SIN_POLY[0] + x2 * (SIN_POLY[1] + x2 * SIN_POLY[2]))
    cosine = 1.0 - 0.5 * x2 + x2 * x2 * (COS_POLY[0] + x2 * (COS_POLY[1] + x2 * COS_POLY[2]))
    quarter = turns.astype(jnp.int32)
    swap = (quarter & 1) == 1
    first, second = jnp.where(swap, sine, cosine), jnp.where(swap, cosine, sine)
    return jnp.where(((quarter + 1) & 2) == 2, -first, first), jnp.where((quarter & 2) == 2, -second, second)


def multicast_kernel(plan, group_size, buf_in, scale_ref, wq_ref, wk_ref, wv_ref, pos_ref, freq_ref, buf, lin, cos_out, sin_out, got, ring_sem, pair_sem, fresh, made, turned, in_sem, out_sem, turn_sem):
    del buf_in
    chips = group_size // CORES
    me = lax.axis_index("tp")
    chip, core = lax.div(me, CORES), lax.rem(me, CORES)
    mate = chip * CORES + (1 - core)
    step = 1 - 2 * core

    def chip_at(delta):
        return lax.rem(chip + delta * step + 2 * chips, chips)

    ahead, behind = chip_at(1) * CORES + core, chip_at(-1) * CORES + core

    barrier = pltpu.get_barrier_semaphore()
    for other in (mate, ahead, behind):
        pl.semaphore_signal(barrier, inc=1, device_id={"tp": other}, device_id_type=pl.DeviceIdType.MESH)
    pl.semaphore_wait(barrier, 3)

    own_n = [c // CHUNK for c in plan.caps]
    own_n[0] += plan.hot // CHUNK
    own_at, at = [], 0
    for c in own_n:
        own_at.append(at)
        at += c
    first = [own_at[2 * c] for c in range(chips)]
    half = [(own_n[2 * c] + own_n[2 * c + 1]) // 2 for c in range(chips)]
    turn = [own_n[2 * c] - half[c] for c in range(chips)]

    def rows(j):
        return pl.ds(pl.multiple_of(j * CHUNK, CHUNK), CHUNK)

    def ring(j):
        return pltpu.make_async_remote_copy(src_ref=buf.at[rows(j)], dst_ref=buf.at[rows(j)], send_sem=ring_sem.at[j], recv_sem=got.at[j], device_id={"tp": ahead}, device_id_type=pl.DeviceIdType.MESH)

    def pair(j):
        return pltpu.make_async_remote_copy(src_ref=buf.at[rows(j)], dst_ref=buf.at[rows(j)], send_sem=pair_sem.at[j], recv_sem=got.at[j], device_id={"tp": mate}, device_id_type=pl.DeviceIdType.MESH)

    def loop(count, fn):
        def body(t, c):
            fn(t)
            return c
        lax.fori_loop(0, count, body, 0)

    my_first, my_half, my_turn = choose(first, chip), choose(half, chip), choose(turn, chip)
    mine = jnp.where(core == 0, my_half, my_half - my_turn)
    mine_at = jnp.where(core == 0, my_first, my_first + my_half + my_turn)
    cross_at = my_first + my_half

    @pl.when(core == 0)
    def _():
        loop(my_turn, lambda t: pair(cross_at + t).start())

    loop(mine, lambda t: ring(mine_at + t).start())
    loop(mine, lambda t: pair(mine_at + t).start())

    @pl.when(core == 1)
    def _():
        def relay(t):
            pair(cross_at + t).wait_recv()
            ring(cross_at + t).start()
        loop(my_turn, relay)

    def arrival(t, way, ring_core):
        chunk, hops, at = jnp.int32(0), jnp.int32(1), jnp.int32(0)
        for hop in range(1, chips):
            origin = lax.rem(chip - hop * way + 2 * chips, chips)
            count = choose(half, origin)
            here = choose(first, origin) + ring_core * count + lax.rem(jnp.maximum(t - at, 0) + ring_core * choose(turn, origin), count)
            chunk = jnp.where(t >= at, here, chunk)
            hops = jnp.where(t >= at, hop, hops)
            at = at + count
        return chunk, hops

    both = my_half * 2
    rot = core * (my_half + my_turn)
    width = 2 * CHUNK

    def home(s, side):
        return my_first + lax.rem(2 * s + side + rot, both)

    def chunks_of(s):
        t = jnp.maximum(s - my_half, 0)
        local = s < my_half
        come, _ = arrival(t, step, core)
        cross, _ = arrival(t, -step, 1 - core)
        return jnp.where(local, home(s, 0), come), jnp.where(local, home(s, 1), cross)

    def load(s, side, j):
        place = lax.rem(s, 2)
        return pltpu.make_async_copy(buf.at[rows(j)], fresh.at[place, pl.ds(side * CHUNK, CHUNK)], in_sem.at[place, side])

    def save(s, side, j):
        place = lax.rem(s, 2)
        at = pl.multiple_of(j * (CHUNK * 8), CHUNK * 8)
        return pltpu.make_async_copy(made.at[place, pl.ds(side * CHUNK * 8, CHUNK * 8)], lin.at[pl.ds(at, CHUNK * 8)], out_sem.at[place, side])

    def compute(s):
        place = lax.rem(s, 2)
        one, two = chunks_of(s)
        load(s, 0, one).wait()
        load(s, 1, two).wait()

        @pl.when(s >= 2)
        def _():
            save(s, 0, 0).wait()
            save(s, 1, 0).wait()
        normed = rms_norm(fresh[place], scale_ref[...])
        at = 0
        for w in (wq_ref, wk_ref, wv_ref):
            y = jnp.dot(normed, w[...], preferred_element_type=jnp.float32).astype(jnp.bfloat16).astype(jnp.float32)
            for j in range(y.shape[1] // 128):
                made[place, pl.ds(at, width, stride=8), :] = y[:, j * 128:(j + 1) * 128]
                at += 1
        save(s, 0, one).start()
        save(s, 1, two).start()

    blocks, span = pos_ref.shape

    def keep(s, which):
        place = lax.rem(s, 2)
        at = pl.multiple_of(s * span, span)
        return pltpu.make_async_copy(turned.at[place, which], (cos_out, sin_out)[which].at[pl.ds(at, span)], turn_sem.at[place, which])

    def tables(s):
        place = lax.rem(s, 2)

        @pl.when(s >= 2)
        def _():
            for which in range(2):
                keep(s - 2, which).wait()
        pos = pos_ref[pl.ds(s, 1), :]
        sub = lax.broadcasted_iota(jnp.int32, (16, span), 0)
        digits = jnp.where(sub == 0, (pos >> 7) << 7, jnp.where(sub == 1, pos & 127, 0))
        digits = digits.astype(jnp.float32).astype(jnp.bfloat16)
        ones = jnp.ones((16, freq_ref.shape[1]), jnp.bfloat16)
        spread = lax.dot_general(digits, ones, (((0,), (0,)), ((), ())), preferred_element_type=jnp.float32)
        cosines, sines = cos_sin(spread * freq_ref[...])
        turned[place, 0] = cosines
        turned[place, 1] = sines
        for which in range(2):
            keep(s, which).start()

    def turn_of(s, carry):
        one, two = chunks_of(s)
        for side, j in ((0, one), (1, two)):
            place = j - my_first
            unseen = jnp.where(core == 0, place >= my_half + my_turn, place < my_half)

            @pl.when((s < my_half) & unseen)
            def _():
                pair(j).wait_recv()

        @pl.when(s >= my_half)
        def _():
            _, hops = arrival(s - my_half, step, core)
            ring(one).wait_recv()

            @pl.when(hops < chips - 1)
            def _():
                ring(one).start()
            pair(one).start()
            pair(two).wait_recv()
        load(s, 0, one).start()
        load(s, 1, two).start()

        @pl.when(s >= 1)
        def _():
            compute(s - 1)

        @pl.when(s < blocks)
        def _():
            tables(s)
        return carry

    rounds = plan.rows // CHUNK // 2
    assert 2 <= blocks <= rounds
    lax.fori_loop(0, rounds, turn_of, 0)
    compute(jnp.int32(rounds - 1))
    for s in (rounds - 2, rounds - 1):
        for side in range(2):
            save(jnp.int32(s), side, 0).wait()
    for s in (blocks - 2, blocks - 1):
        for which in range(2):
            keep(jnp.int32(s), which).wait()

    @pl.when(core == 0)
    def _():
        loop(my_turn, lambda t: pair(cross_at + t).wait_send())

    @pl.when(core == 1)
    def _():
        loop(my_turn, lambda t: ring(cross_at + t).wait_send())

    def sent(t):
        ring(mine_at + t).wait_send()
        pair(mine_at + t).wait_send()
    loop(mine, sent)
    for hop in range(1, chips):
        origin = chip_at(-hop)
        count = choose(half, origin)
        base = choose(first, origin) + core * count

        def left(t):
            if hop < chips - 1:
                ring(base + t).wait_send()
            pair(base + t).wait_send()
        loop(count, left)


def multicast(plan, group_size, buf, norm_scale, w_query, key_cols, value_cols, positions):
    chunks, width = plan.rows // CHUNK, buf.shape[1]
    tokens, half = positions.shape[0], HEAD_DIM // 2
    table = jax.ShapeDtypeStruct((tokens, half), jnp.float32)
    vmem = pl.BlockSpec(memory_space=pltpu.VMEM)
    return pl.pallas_call(
        functools.partial(multicast_kernel, plan, group_size),
        out_shape=(jax.ShapeDtypeStruct(buf.shape, buf.dtype), jax.ShapeDtypeStruct((plan.rows * 8, 128), jnp.float32), table, table),
        in_specs=[pl.BlockSpec(memory_space=pl.ANY)] + [vmem] * 6,
        out_specs=(pl.BlockSpec(memory_space=pl.ANY),) * 4,
        scratch_shapes=[
            pltpu.SemaphoreType.DMA((chunks,)),
            pltpu.SemaphoreType.DMA((chunks,)),
            pltpu.SemaphoreType.DMA((chunks,)),
            pltpu.VMEM((2, 2 * CHUNK, width), buf.dtype),
            pltpu.VMEM((2, 2 * CHUNK * 8, 128), jnp.float32),
            pltpu.VMEM((2, 2, TURN, half), jnp.float32),
            pltpu.SemaphoreType.DMA((2, 2)),
            pltpu.SemaphoreType.DMA((2, 2)),
            pltpu.SemaphoreType.DMA((2, 2)),
        ],
        input_output_aliases={0: 0},
        compiler_params=pltpu.CompilerParams(collective_id=0, has_side_effects=True, vmem_limit_bytes=VMEM_LIMIT),
        cost_estimate=pl.CostEstimate(flops=100_000_000_000, bytes_accessed=100_000_000, transcendentals=0),
        name="multicast",
    )(buf, norm_scale.reshape(1, width), w_query, key_cols, value_cols, positions.reshape(-1, TURN), inverse_freq().reshape(1, half))


def expand_kernel(lag, slots, lin, source, slots_ref, cos_ref, sin_ref, r_ref, q_ref, k_ref, v_ref, store, spread, slabs, offsets, sem, fetch_sem):
    step, steps = pl.program_id(0), pl.num_programs(0) - lag
    me = lax.axis_index("tp")
    whole = pltpu.make_async_copy(lin, store, sem)
    picks = r_ref.shape[0] // PICK
    picker = Picker(slots, me * (steps * picks * PICK), steps * picks, offsets, source, slabs, fetch_sem)

    @pl.when(step == 0)
    def _():
        whole.start()
        picker.lead()
        lines = steps * picks * PICK // 128
        offsets[...] = offsets_by_column(slots_ref[pl.ds(pl.multiple_of(me * lines, 8), 8), :])

    @pl.when(step < steps)
    def _():
        for i in range(picks):
            r_ref[pl.ds(i * PICK, PICK), :] = picker.turn(step * picks + i).astype(r_ref.dtype)

    @pl.when(step == steps)
    def _():
        picker.drain(steps * picks)

    @pl.when(step == lag)
    def _():
        whole.wait()

    @pl.when(step >= lag)
    def _():
        def body(b, carry):
            for i in range(32):
                t = b * 32 + i
                at = pl.multiple_of(slots[(step - lag) * TOK + t] * 8, 8)
                spread[pl.ds(pl.multiple_of(t * 8, 8), 8), :] = store[pl.ds(at, 8), :]
            return carry

        lax.fori_loop(0, TOK // 32, body, 0)
        cosines, sines = cos_ref[...], sin_ref[...]
        parts = [spread[pl.ds(j, TOK, stride=8), :] for j in range(6)]
        factor = HEAD_DIM ** -0.5
        half = HEAD_DIM // 2
        q_ref[:, :half] = ((parts[0] * cosines - parts[1] * sines) * factor).astype(q_ref.dtype)
        q_ref[:, half:] = ((parts[1] * cosines + parts[0] * sines) * factor).astype(q_ref.dtype)
        k_ref[:, :half] = (parts[2] * cosines - parts[3] * sines).astype(k_ref.dtype)
        k_ref[:, half:] = (parts[3] * cosines + parts[2] * sines).astype(k_ref.dtype)
        v_ref[:, :half] = parts[4].astype(v_ref.dtype)
        v_ref[:, half:] = parts[5].astype(v_ref.dtype)


def expand(group_size, lin, source, slots, cosines, sines):
    tokens, width = slots.shape[0] * slots.shape[1], source.shape[1]
    steps, mine = tokens // TOK, tokens // group_size
    lag = LAG
    assert mine % (steps * PICK) == 0 and mine == 8 * 128
    head = jax.ShapeDtypeStruct((tokens, HEAD_DIM), jnp.bfloat16)
    late = lambda i, s: (jnp.maximum(i - lag, 0), 0)
    return pl.pallas_call(
        functools.partial(expand_kernel, lag),
        grid_spec=pltpu.PrefetchScalarGridSpec(
            num_scalar_prefetch=1,
            grid=(steps + lag,),
            in_specs=[
                pl.BlockSpec(memory_space=pl.ANY),
                pl.BlockSpec(memory_space=pl.ANY),
                pl.BlockSpec(memory_space=pltpu.VMEM),
                pl.BlockSpec((TOK, HEAD_DIM // 2), late),
                pl.BlockSpec((TOK, HEAD_DIM // 2), late),
            ],
            out_specs=[pl.BlockSpec((mine // steps, width), lambda i, s: (jnp.minimum(i, steps - 1), 0))] + [pl.BlockSpec((TOK, HEAD_DIM), late)] * 3,
            scratch_shapes=[
                pltpu.VMEM(lin.shape, lin.dtype),
                pltpu.VMEM((TOK * 8, 128), jnp.float32),
                pltpu.VMEM((DEPTH, PICK * SLAB, width), source.dtype),
                pltpu.VMEM((128, 128), jnp.float32),
                pltpu.SemaphoreType.DMA,
                pltpu.SemaphoreType.DMA((DEPTH,)),
            ],
        ),
        out_shape=(jax.ShapeDtypeStruct((mine, width), source.dtype),) + (head,) * 3,
        compiler_params=pltpu.CompilerParams(vmem_limit_bytes=VMEM_LIMIT),
        name="expand",
    )(slots.reshape(tokens), lin, source, slots, cosines, sines)


def solution(mesh):
    group_size = mesh.shape["tp"]

    def local_step(token_ids, positions, table_rows, norm_scale, w_query, w_key, w_value):
        dev_index = lax.axis_index("tp")
        vocab_rows, model_width = table_rows.shape
        tokens = token_ids.shape[0]
        normalizer = float(np.asarray(math.sqrt(model_width), dtype=jnp.bfloat16))
        kv_heads = w_key.shape[1] // HEAD_DIM
        slot_count = max(kv_heads, group_size)
        slots_here = slot_count // group_size
        first_head = (dev_index * slots_here) // (slot_count // kv_heads)
        if kv_heads * HEAD_DIM == slots_here * HEAD_DIM:
            key_cols, value_cols = w_key, w_value
        else:
            key_cols = lax.dynamic_slice_in_dim(w_key, first_head * HEAD_DIM, slots_here * HEAD_DIM, axis=1)
            value_cols = lax.dynamic_slice_in_dim(w_value, first_head * HEAD_DIM, slots_here * HEAD_DIM, axis=1)

        plan = Plan(group_size, tokens, vocab_rows)
        slots, rows, counts, offsets = prepare(plan, group_size, vocab_rows, token_ids)
        fits = counts[group_size, 0] <= 0
        buf = gather_rows(plan, normalizer, counts, rows.reshape(-1), offsets, table_rows)
        buf, lin, cosines, sines = multicast(plan, group_size, buf, norm_scale, w_query, key_cols, value_cols, positions)

        def fast(buf, lin, cosines, sines):
            return expand(group_size, lin, buf, slots, cosines, sines)

        def slow(buf, lin, cosines, sines):
            return dense_path(group_size, token_ids, positions, table_rows, norm_scale, w_query, key_cols, value_cols)

        residual, queries, key_heads, value_heads = lax.cond(fits, fast, slow, buf, lin, cosines, sines)
        return residual, queries[:, None, :], key_heads[:, None, :], value_heads[:, None, :]

    head_spec = P("dp", "tp", None)
    return jax.shard_map(local_step, mesh=mesh, in_specs=(P("dp"), P("dp"), P("tp", None), P(), P(None, "tp"), P(), P()), out_specs=(P(("dp", "tp"), None), head_spec, head_spec, head_spec), check_vma=False)
```

```python
import functools
import math
import jax
import jax.numpy as jnp
import numpy as np
from jax import lax
from jax.experimental import pallas as pl
from jax.experimental.pallas import tpu as pltpu
from jax.sharding import PartitionSpec as P

HEAD_DIM = 256
EPSILON = 1e-6
ROPE_BASE = 10000.0
CHUNK = 64
PICK = 64
SLAB = 8
DEPTH = 4
CORES = 2
VMEM_LIMIT = 60 * 1024 * 1024


def inverse_freq():
    return ROPE_BASE ** (-jnp.arange(0, HEAD_DIM, 2, dtype=jnp.float32) / HEAD_DIM)


def rope_tables(positions):
    angles = positions.astype(jnp.float32)[:, None] * inverse_freq()[None, :]
    return jnp.cos(angles), jnp.sin(angles)


def rms_norm(resid_rows, norm_scale):
    widened = resid_rows.astype(jnp.float32)
    inv_rms = lax.rsqrt(jnp.mean(widened * widened, axis=-1, keepdims=True) + EPSILON)
    return (widened * inv_rms * (1.0 + norm_scale)).astype(jnp.bfloat16)


def rotate(head_vals, cosines, sines):
    half_dim = head_vals.shape[-1] // 2
    front_half = head_vals[..., :half_dim]
    back_half = head_vals[..., half_dim:]
    return jnp.concatenate([front_half * cosines - back_half * sines, back_half * cosines + front_half * sines], axis=-1)


def project(normed, weight, cosines, sines, factor):
    linear = jnp.dot(normed, weight, preferred_element_type=jnp.float32).astype(jnp.bfloat16)
    head_view = linear.reshape(linear.shape[0], -1, HEAD_DIM).astype(jnp.float32)
    return (rotate(head_view, cosines, sines) * factor).astype(jnp.bfloat16)


def dense_path(group_size, token_ids, positions, table_rows, norm_scale, w_query, key_cols, value_cols):
    dev_index = lax.axis_index("tp")
    vocab_rows, model_width = table_rows.shape
    normalizer = jnp.asarray(math.sqrt(model_width), dtype=jnp.bfloat16)
    local_ids = token_ids - dev_index * vocab_rows
    inside = (local_ids >= 0) & (local_ids < vocab_rows)
    picked = jnp.take(table_rows, local_ids, axis=0, mode="clip") * normalizer
    partial = jnp.where(inside[:, None], picked, jnp.zeros((), jnp.bfloat16))
    by_owner = partial.reshape(group_size, -1, model_width)
    residual = jnp.sum(lax.all_to_all(by_owner, "tp", 0, 0), axis=0)
    normed = rms_norm(residual, norm_scale)
    copies = jnp.broadcast_to(normed[None], (group_size, *normed.shape))
    normed = lax.all_to_all(copies, "tp", 0, 0).reshape(-1, model_width)
    cosines, sines = rope_tables(positions)
    cosines, sines = cosines[:, None, :], sines[:, None, :]
    queries = project(normed, w_query, cosines, sines, HEAD_DIM ** -0.5)
    key_heads = project(normed, key_cols, cosines, sines, 1.0)
    value_lin = jnp.dot(normed, value_cols, preferred_element_type=jnp.float32).astype(jnp.bfloat16)
    return residual, queries[:, 0, :], key_heads[:, 0, :], value_lin


class Plan:
    def __init__(self, group_size, tokens, vocab_rows):
        unit = CHUNK * 2
        self.hot = min(tokens // 8, vocab_rows // unit * unit)
        share = [11 / 32, 5 / 64] + [3 / 64] * 2
        room = [share[o] if o < 4 else 3 / 128 for o in range(group_size)]
        self.caps = [max(CHUNK, -(-int(tokens * r) // CHUNK) * CHUNK) for r in room]
        self.bases, at = [], self.hot
        for cap in self.caps:
            self.bases.append(at)
            at += cap
        self.rows = at
        self.list_rows = -(-(-(-max(self.caps) // 128)) // 8) * 8


def choose(values, index):
    out = jnp.int32(values[0])
    for j in range(1, len(values)):
        out = jnp.where(index == j, jnp.int32(values[j]), out)
    return out


def offsets_by_column(rows):
    offsets = (rows & (SLAB - 1)).astype(jnp.float32)
    fill = jnp.zeros((128 - rows.shape[0], 128), jnp.float32)
    return jnp.concatenate([offsets, fill], axis=0).T


def prep_kernel(plan, group_size, vocab_rows, ids_ref, slot_ref, list_ref, count_ref, offset_ref, over_ref):
    me = lax.axis_index("tp")
    ids = ids_ref[...]
    blocks, lanes = ids.shape
    cold = ids >= plan.hot
    masks = [cold & (ids >= o * vocab_rows) & (ids < (o + 1) * vocab_rows) for o in range(group_size)]
    stack = jnp.concatenate([m.astype(jnp.float32) for m in masks], axis=0)
    stack = stack.astype(jnp.bfloat16)
    tri_r = lax.broadcasted_iota(jnp.int32, (lanes, lanes), 0)
    tri_c = lax.broadcasted_iota(jnp.int32, (lanes, lanes), 1)
    upper = (tri_r <= tri_c).astype(jnp.float32).astype(jnp.bfloat16)
    within = jnp.dot(stack, upper, preferred_element_type=jnp.float32)
    totals = jnp.dot(stack, jnp.ones((lanes, lanes), jnp.bfloat16), preferred_element_type=jnp.float32)
    low_r = lax.broadcasted_iota(jnp.int32, (blocks, blocks), 0)
    low_c = lax.broadcasted_iota(jnp.int32, (blocks, blocks), 1)
    lower = (low_c < low_r).astype(jnp.float32).astype(jnp.bfloat16)
    slot = jnp.where(cold, 0, ids)
    own_rank = jnp.full((blocks, lanes), -1, jnp.int32)
    over = jnp.zeros((1, lanes), jnp.int32)
    for o in range(group_size):
        tot = totals[o * blocks:(o + 1) * blocks]
        before = jnp.dot(lower, tot.astype(jnp.bfloat16), preferred_element_type=jnp.float32)
        rank = (before + within[o * blocks:(o + 1) * blocks]).astype(jnp.int32) - 1
        slot = slot + jnp.where(masks[o], jnp.minimum(rank, plan.caps[o] - 1) + plan.bases[o], 0)
        own_rank = jnp.where(masks[o] & (me == o), rank, own_rank)
        count = (before[blocks - 1:] + tot[blocks - 1:]).astype(jnp.int32)
        count_ref[o:o + 1, :] = count
        over = jnp.maximum(over, count - plan.caps[o])
    slot_ref[...] = slot
    over_ref[0] = jnp.max(over)
    local = jnp.where(own_rank >= 0, ids - me * vocab_rows, 0)
    major, minor = own_rank >> 7, own_rank & 127
    high, low = local >> 8, local & 255
    iota_major = lax.broadcasted_iota(jnp.int32, (plan.list_rows, lanes), 0)
    iota_minor = lax.broadcasted_iota(jnp.int32, (lanes, lanes), 0)
    acc = jnp.zeros((2 * plan.list_rows, lanes), jnp.float32)
    per = 8
    for g in range(blocks // per):
        lhs, rhs = [], []
        for r in range(g * per, (g + 1) * per):
            hit = iota_major == major[r:r + 1, :]
            lhs.append(jnp.concatenate([jnp.where(hit, high[r:r + 1, :], 0), jnp.where(hit, low[r:r + 1, :], 0)], axis=0).astype(jnp.float32))
            rhs.append((iota_minor == minor[r:r + 1, :]).astype(jnp.float32))
        left = jnp.concatenate(lhs, axis=1).astype(jnp.bfloat16)
        right = jnp.concatenate(rhs, axis=1).astype(jnp.bfloat16)
        acc = acc + lax.dot_general(left, right, (((1,), (1,)), ((), ())), preferred_element_type=jnp.float32)
    whole = acc.astype(jnp.int32)
    wanted = whole[:plan.list_rows] * 256 + whole[plan.list_rows:]
    list_ref[...] = wanted
    offset_ref[...] = offsets_by_column(wanted)


def prepare(plan, group_size, vocab_rows, token_ids):
    blocks = token_ids.shape[0] // 128
    return pl.pallas_call(
        functools.partial(prep_kernel, plan, group_size, vocab_rows),
        out_shape=(
            jax.ShapeDtypeStruct((blocks, 128), jnp.int32),
            jax.ShapeDtypeStruct((plan.list_rows, 128), jnp.int32),
            jax.ShapeDtypeStruct((group_size, 128), jnp.int32),
            jax.ShapeDtypeStruct((128, 128), jnp.float32),
            jax.ShapeDtypeStruct((1,), jnp.int32),
        ),
        out_specs=[pl.BlockSpec(memory_space=pltpu.VMEM)] * 4 + [pl.BlockSpec(memory_space=pltpu.SMEM)],
        compiler_params=pltpu.CompilerParams(vmem_limit_bytes=VMEM_LIMIT),
        name="slots",
    )(token_ids.reshape(blocks, 128))


class Picker:
    def __init__(self, rows_smem, begin, groups, offsets, source, slabs, sem):
        self.rows_smem, self.begin, self.groups = rows_smem, begin, groups
        self.offsets, self.source, self.slabs, self.sem = offsets, source, slabs, sem

    def fetch(self, g):
        place = lax.rem(jnp.int32(g), DEPTH)
        first = self.begin + jnp.minimum(g, jnp.maximum(self.groups - 1, 0)) * PICK
        for i in range(PICK):
            row = self.rows_smem[first + i]
            start = pl.multiple_of((row >> 3) << 3, SLAB)
            pltpu.make_async_copy(self.source.at[pl.ds(start, SLAB)], self.slabs.at[place, pl.ds(i * SLAB, SLAB)], self.sem.at[place]).start()

    def wait(self, g):
        place = lax.rem(jnp.int32(g), DEPTH)
        pltpu.make_async_copy(self.source.at[pl.ds(0, PICK * SLAB)], self.slabs.at[place], self.sem.at[place]).wait()

    def pick(self, g):
        place = lax.rem(jnp.int32(g), DEPTH)
        per = 128 // PICK
        block = self.offsets[pl.ds(pl.multiple_of(lax.rem(g, per) * PICK, PICK), PICK), :]
        lane = lax.broadcasted_iota(jnp.int32, (PICK, 128), 1)
        column = jnp.sum(jnp.where(lane == lax.div(g, per), block, 0.0), axis=1, keepdims=True).astype(jnp.int32)
        shape = (PICK, PICK * SLAB)
        hit = lax.broadcasted_iota(jnp.int32, shape, 1) == lax.broadcasted_iota(jnp.int32, shape, 0) * SLAB + column
        onehot = jnp.where(hit, 1.0, 0.0).astype(jnp.bfloat16)
        return jnp.dot(onehot, self.slabs[place], preferred_element_type=jnp.float32)

    def lead(self):
        for g in range(DEPTH - 1):
            self.fetch(g)

    def turn(self, g):
        self.wait(g)
        self.fetch(g + DEPTH - 1)
        return self.pick(g)

    def drain(self, groups):
        for g in range(DEPTH - 1):
            self.wait(groups + g)


def gather_kernel(plan, normalizer, counts, rows_smem, offsets, table, out, slabs, stage, hot_in, hot_out, sem, out_sem, hot_sem):
    me = lax.axis_index("tp")
    total = jnp.minimum(counts[me, 0], choose(plan.caps, me))
    base = choose(plan.bases, me)
    scale = jnp.float32(normalizer)
    groups = (total + PICK - 1) // PICK
    picker = Picker(rows_smem, 0, groups, offsets, table, slabs, sem)
    picker.lead()

    def emit(g, picked):
        side = lax.rem(g, 2)

        @pl.when(g >= 2)
        def _():
            pltpu.make_async_copy(stage.at[side], out.at[pl.ds(0, PICK)], out_sem.at[side]).wait()

        stage[side] = (picked * scale).astype(jnp.bfloat16)
        at = pl.multiple_of(base + g * PICK, PICK)
        pltpu.make_async_copy(stage.at[side], out.at[pl.ds(at, PICK)], out_sem.at[side]).start()

    step = hot_in.shape[1]
    hot_steps = jnp.where(me == 0, plan.hot // step, 0)

    def load(i):
        return pltpu.make_async_copy(table.at[pl.ds(pl.multiple_of(i * step, step), step)], hot_in.at[lax.rem(i, 2)], hot_sem.at[lax.rem(i, 2)])

    def save(i):
        return pltpu.make_async_copy(hot_out.at[lax.rem(i, 2)], out.at[pl.ds(pl.multiple_of(i * step, step), step)], hot_sem.at[2 + lax.rem(i, 2)])

    def hot_turn(i):
        @pl.when(i < hot_steps)
        def _():
            load(i).wait()

            @pl.when(i >= 2)
            def _():
                save(i - 2).wait()
            hot_out[lax.rem(i, 2)] = (hot_in[lax.rem(i, 2)].astype(jnp.float32) * scale).astype(jnp.bfloat16)
            save(i).start()

            @pl.when(i + 2 < hot_steps)
            def _():
                load(i + 2).start()

    for i in range(2):
        @pl.when(i < hot_steps)
        def _():
            load(jnp.int32(i)).start()

    def rest(i, carry):
        hot_turn(i)
        return carry

    def body(g, carry):
        emit(g, picker.turn(g))
        hot_turn(g)
        return carry

    lax.fori_loop(0, groups, body, 0)
    lax.fori_loop(groups, jnp.maximum(hot_steps, groups), rest, 0)
    picker.drain(groups)
    for back in (2, 1):
        @pl.when(hot_steps >= back)
        def _():
            save(hot_steps - back).wait()
    for last in (2, 1):
        @pl.when(groups >= last)
        def _():
            side = lax.rem(groups - last, 2)
            pltpu.make_async_copy(stage.at[side], out.at[pl.ds(0, PICK)], out_sem.at[side]).wait()


def gather_rows(plan, normalizer, counts, rows, offsets, table):
    width = table.shape[1]
    hot_step = CHUNK
    return pl.pallas_call(
        functools.partial(gather_kernel, plan, normalizer),
        out_shape=jax.ShapeDtypeStruct((plan.rows, width), table.dtype),
        in_specs=[pl.BlockSpec(memory_space=pltpu.SMEM), pl.BlockSpec(memory_space=pltpu.SMEM), pl.BlockSpec(memory_space=pltpu.VMEM), pl.BlockSpec(memory_space=pl.ANY)],
        out_specs=pl.BlockSpec(memory_space=pl.ANY),
        scratch_shapes=[
            pltpu.VMEM((DEPTH, PICK * SLAB, width), table.dtype),
            pltpu.VMEM((2, PICK, width), table.dtype),
            pltpu.VMEM((2, hot_step, width), table.dtype),
            pltpu.VMEM((2, hot_step, width), table.dtype),
            pltpu.SemaphoreType.DMA((DEPTH,)),
            pltpu.SemaphoreType.DMA((2,)),
            pltpu.SemaphoreType.DMA((4,)),
        ],
        compiler_params=pltpu.CompilerParams(vmem_limit_bytes=VMEM_LIMIT),
        cost_estimate=pl.CostEstimate(flops=2 * 2048 * 256 * 2816, bytes_accessed=100_000_000, transcendentals=0),
        name="owner_rows",
    )(counts, rows, offsets, table)


TOK = 512
SUB = 32
UNROLL = 4
TURN = 256
LAG = 2
HALF_PI = (1.5703125, 4.837512969970703e-4, 7.549789948768648e-8)
SIN_POLY = (-1.6666654611e-1, 8.3321608736e-3, -1.9515295891e-4)
COS_POLY = (4.166664568298827e-2, -1.388731625493765e-3, 2.443315711809948e-5)


def cos_sin(angles):
    turns = jnp.floor(angles * (2 / math.pi) + 0.5)
    x = angles - turns * HALF_PI[0]
    x = x - turns * HALF_PI[1]
    x = x - turns * HALF_PI[2]
    x2 = x * x
    sine = x + x * x2 * (SIN_POLY[0] + x2 * (SIN_POLY[1] + x2 * SIN_POLY[2]))
    cosine = 1.0 - 0.5 * x2 + x2 * x2 * (COS_POLY[0] + x2 * (COS_POLY[1] + x2 * COS_POLY[2]))
    quarter = turns.astype(jnp.int32)
    swap = (quarter & 1) == 1
    first, second = jnp.where(swap, sine, cosine), jnp.where(swap, cosine, sine)
    return jnp.where(((quarter + 1) & 2) == 2, -first, first), jnp.where((quarter & 2) == 2, -second, second)


def multicast_kernel(plan, group_size, buf_in, scale_ref, wq_ref, wk_ref, wv_ref, pos_ref, freq_ref, buf, lin, tiles, cos_out, sin_out, got, ring_sem, pair_sem, fresh, made, wide, tiled, turned, in_sem, out_sem, tile_sem, turn_sem):
    del buf_in
    chips = group_size // CORES
    me = lax.axis_index("tp")
    chip, core = lax.div(me, CORES), lax.rem(me, CORES)
    mate = chip * CORES + (1 - core)
    step = 1 - 2 * core

    def chip_at(delta):
        return lax.rem(chip + delta * step + 2 * chips, chips)

    ahead, behind = chip_at(1) * CORES + core, chip_at(-1) * CORES + core

    barrier = pltpu.get_barrier_semaphore()
    for other in (mate, ahead, behind):
        pl.semaphore_signal(barrier, inc=1, device_id={"tp": other}, device_id_type=pl.DeviceIdType.MESH)
    pl.semaphore_wait(barrier, 3)

    own_n = [c // CHUNK for c in plan.caps]
    own_n[0] += plan.hot // CHUNK
    own_at, at = [], 0
    for c in own_n:
        own_at.append(at)
        at += c
    first = [own_at[2 * c] for c in range(chips)]
    half = [(own_n[2 * c] + own_n[2 * c + 1]) // 2 for c in range(chips)]
    turn = [own_n[2 * c] - half[c] for c in range(chips)]

    def rows(j):
        return pl.ds(pl.multiple_of(j * CHUNK, CHUNK), CHUNK)

    def ring(j):
        return pltpu.make_async_remote_copy(src_ref=buf.at[rows(j)], dst_ref=buf.at[rows(j)], send_sem=ring_sem.at[j], recv_sem=got.at[j], device_id={"tp": ahead}, device_id_type=pl.DeviceIdType.MESH)

    def pair(j):
        return pltpu.make_async_remote_copy(src_ref=buf.at[rows(j)], dst_ref=buf.at[rows(j)], send_sem=pair_sem.at[j], recv_sem=got.at[j], device_id={"tp": mate}, device_id_type=pl.DeviceIdType.MESH)

    def loop(count, fn):
        def body(t, c):
            fn(t)
            return c
        lax.fori_loop(0, count, body, 0)

    my_first, my_half, my_turn = choose(first, chip), choose(half, chip), choose(turn, chip)
    mine = jnp.where(core == 0, my_half, my_half - my_turn)
    mine_at = jnp.where(core == 0, my_first, my_first + my_half + my_turn)
    cross_at = my_first + my_half

    @pl.when(core == 0)
    def _():
        loop(my_turn, lambda t: pair(cross_at + t).start())

    loop(mine, lambda t: ring(mine_at + t).start())
    loop(mine, lambda t: pair(mine_at + t).start())

    @pl.when(core == 1)
    def _():
        def relay(t):
            pair(cross_at + t).wait_recv()
            ring(cross_at + t).start()
        loop(my_turn, relay)

    def arrival(t, way, ring_core):
        chunk, hops, at = jnp.int32(0), jnp.int32(1), jnp.int32(0)
        for hop in range(1, chips):
            origin = lax.rem(chip - hop * way + 2 * chips, chips)
            count = choose(half, origin)
            here = choose(first, origin) + ring_core * count + lax.rem(jnp.maximum(t - at, 0) + ring_core * choose(turn, origin), count)
            chunk = jnp.where(t >= at, here, chunk)
            hops = jnp.where(t >= at, hop, hops)
            at = at + count
        return chunk, hops

    both = my_half * 2
    rot = core * (my_half + my_turn)
    width = 2 * CHUNK

    def home(s, side):
        return my_first + lax.rem(2 * s + side + rot, both)

    def chunks_of(s):
        t = jnp.maximum(s - my_half, 0)
        local = s < my_half
        come, _ = arrival(t, step, core)
        cross, _ = arrival(t, -step, 1 - core)
        return jnp.where(local, home(s, 0), come), jnp.where(local, home(s, 1), cross)

    def load(s, side, j):
        place = lax.rem(s, 2)
        return pltpu.make_async_copy(buf.at[rows(j)], fresh.at[place, pl.ds(side * CHUNK, CHUNK)], in_sem.at[place, side])

    def save(s, side, j):
        place = lax.rem(s, 2)
        at = pl.multiple_of(j * (CHUNK * 8), CHUNK * 8)
        return pltpu.make_async_copy(made.at[place, pl.ds(side * CHUNK * 8, CHUNK * 8)], lin.at[pl.ds(at, CHUNK * 8)], out_sem.at[place, side])

    per_row = tiles.shape[0] // plan.rows

    def lay(s, side, j):
        place = lax.rem(s, 2)
        at = pl.multiple_of(j * (CHUNK * per_row), CHUNK * per_row)
        return pltpu.make_async_copy(tiled.at[place, pl.ds(side * CHUNK * per_row, CHUNK * per_row)], tiles.at[pl.ds(at, CHUNK * per_row)], tile_sem.at[place, side])

    def compute(s):
        place = lax.rem(s, 2)
        one, two = chunks_of(s)
        load(s, 0, one).wait()
        load(s, 1, two).wait()

        @pl.when(s >= 2)
        def _():
            save(s, 0, 0).wait()
            save(s, 1, 0).wait()
            lay(s, 0, 0).wait()
            lay(s, 1, 0).wait()
        came = fresh[place]
        for j in range(per_row):
            wide[pl.ds(j, width, stride=per_row), :] = came[:, j * 128:(j + 1) * 128].astype(jnp.float32)
        tiled[place] = wide[...].astype(tiled.dtype)
        lay(s, 0, one).start()
        lay(s, 1, two).start()
        normed = rms_norm(came, scale_ref[...])
        at = 0
        for w in (wq_ref, wk_ref, wv_ref):
            y = jnp.dot(normed, w[...], preferred_element_type=jnp.float32).astype(jnp.bfloat16).astype(jnp.float32)
            for j in range(y.shape[1] // 128):
                made[place, pl.ds(at, width, stride=8), :] = y[:, j * 128:(j + 1) * 128]
                at += 1
        save(s, 0, one).start()
        save(s, 1, two).start()

    lines, span = TURN // 128, TURN
    blocks = pos_ref.shape[0] // lines

    def keep(s, which):
        place = lax.rem(s, 2)
        at = pl.multiple_of(s * span, span)
        return pltpu.make_async_copy(turned.at[place, which], (cos_out, sin_out)[which].at[pl.ds(at, span)], turn_sem.at[place, which])

    def tables(s):
        place = lax.rem(s, 2)

        @pl.when(s >= 2)
        def _():
            for which in range(2):
                keep(s - 2, which).wait()
        pos = jnp.concatenate([pos_ref[pl.ds(s * lines + i, 1), :] for i in range(lines)], axis=1)
        sub = lax.broadcasted_iota(jnp.int32, (16, span), 0)
        digits = jnp.where(sub == 0, (pos >> 7) << 7, jnp.where(sub == 1, pos & 127, 0))
        digits = digits.astype(jnp.float32).astype(jnp.bfloat16)
        ones = jnp.ones((16, freq_ref.shape[1]), jnp.bfloat16)
        spread = lax.dot_general(digits, ones, (((0,), (0,)), ((), ())), preferred_element_type=jnp.float32)
        cosines, sines = cos_sin(spread * freq_ref[...])
        turned[place, 0] = cosines
        turned[place, 1] = sines
        for which in range(2):
            keep(s, which).start()

    def turn_of(s, carry):
        one, two = chunks_of(s)
        for side, j in ((0, one), (1, two)):
            place = j - my_first
            unseen = jnp.where(core == 0, place >= my_half + my_turn, place < my_half)

            @pl.when((s < my_half) & unseen)
            def _():
                pair(j).wait_recv()

        @pl.when(s >= my_half)
        def _():
            _, hops = arrival(s - my_half, step, core)
            ring(one).wait_recv()

            @pl.when(hops < chips - 1)
            def _():
                ring(one).start()
            pair(one).start()
            pair(two).wait_recv()
        load(s, 0, one).start()
        load(s, 1, two).start()

        @pl.when(s >= 1)
        def _():
            compute(s - 1)

        @pl.when(s < blocks)
        def _():
            tables(s)
        return carry

    rounds = plan.rows // CHUNK // 2
    assert 2 <= blocks <= rounds
    lax.fori_loop(0, rounds, turn_of, 0)
    compute(jnp.int32(rounds - 1))
    for s in (rounds - 2, rounds - 1):
        for side in range(2):
            save(jnp.int32(s), side, 0).wait()
            lay(jnp.int32(s), side, 0).wait()
    for s in (blocks - 2, blocks - 1):
        for which in range(2):
            keep(jnp.int32(s), which).wait()

    @pl.when(core == 0)
    def _():
        loop(my_turn, lambda t: pair(cross_at + t).wait_send())

    @pl.when(core == 1)
    def _():
        loop(my_turn, lambda t: ring(cross_at + t).wait_send())

    def sent(t):
        ring(mine_at + t).wait_send()
        pair(mine_at + t).wait_send()
    loop(mine, sent)
    for hop in range(1, chips):
        origin = chip_at(-hop)
        count = choose(half, origin)
        base = choose(first, origin) + core * count

        def left(t):
            if hop < chips - 1:
                ring(base + t).wait_send()
            pair(base + t).wait_send()
        loop(count, left)


def multicast(plan, group_size, buf, norm_scale, w_query, key_cols, value_cols, positions):
    chunks, width = plan.rows // CHUNK, buf.shape[1]
    per_row = width // 128
    tokens, half = positions.shape[0], HEAD_DIM // 2
    table = jax.ShapeDtypeStruct((tokens, half), jnp.float32)
    vmem = pl.BlockSpec(memory_space=pltpu.VMEM)
    return pl.pallas_call(
        functools.partial(multicast_kernel, plan, group_size),
        out_shape=(jax.ShapeDtypeStruct(buf.shape, buf.dtype), jax.ShapeDtypeStruct((plan.rows * 8, 128), jnp.float32), jax.ShapeDtypeStruct((plan.rows * per_row, 128), buf.dtype), table, table),
        in_specs=[pl.BlockSpec(memory_space=pl.ANY)] + [vmem] * 6,
        out_specs=(pl.BlockSpec(memory_space=pl.ANY),) * 5,
        scratch_shapes=[
            pltpu.SemaphoreType.DMA((chunks,)),
            pltpu.SemaphoreType.DMA((chunks,)),
            pltpu.SemaphoreType.DMA((chunks,)),
            pltpu.VMEM((2, 2 * CHUNK, width), buf.dtype),
            pltpu.VMEM((2, 2 * CHUNK * 8, 128), jnp.float32),
            pltpu.VMEM((2 * CHUNK * per_row, 128), jnp.float32),
            pltpu.VMEM((2, 2 * CHUNK * per_row, 128), buf.dtype),
            pltpu.VMEM((2, 2, TURN, half), jnp.float32),
            pltpu.SemaphoreType.DMA((2, 2)),
            pltpu.SemaphoreType.DMA((2, 2)),
            pltpu.SemaphoreType.DMA((2, 2)),
            pltpu.SemaphoreType.DMA((2, 2)),
        ],
        input_output_aliases={0: 0},
        compiler_params=pltpu.CompilerParams(collective_id=0, has_side_effects=True, vmem_limit_bytes=VMEM_LIMIT),
        cost_estimate=pl.CostEstimate(flops=100_000_000_000, bytes_accessed=100_000_000, transcendentals=0),
        name="multicast",
    )(buf, norm_scale.reshape(1, width), w_query, key_cols, value_cols, positions.reshape(-1, 128), inverse_freq().reshape(1, half))


def expand_kernel(lag, slots, lin, tiles, cos_ref, sin_ref, r_ref, q_ref, k_ref, v_ref, store, spread, raw, wide, sem, fetch_sem):
    step, steps = pl.program_id(0), pl.num_programs(0) - lag
    me = lax.axis_index("tp")
    whole = pltpu.make_async_copy(lin, store, sem)
    count, width = r_ref.shape
    per_row = width // 128

    def fetch(g):
        place = lax.rem(jnp.int32(g), DEPTH)
        first = (me * steps + jnp.minimum(g, steps - 1)) * count
        for i in range(count):
            at = pl.multiple_of(slots[first + i] * per_row, per_row)
            pltpu.make_async_copy(tiles.at[pl.ds(at, per_row)], raw.at[place, pl.ds(i * per_row, per_row)], fetch_sem.at[place]).start()

    def arrived(g):
        place = lax.rem(jnp.int32(g), DEPTH)
        pltpu.make_async_copy(tiles.at[pl.ds(0, count * per_row)], raw.at[place], fetch_sem.at[place]).wait()

    @pl.when(step == 0)
    def _():
        for g in range(DEPTH - 1):
            fetch(g)
        whole.start()

    @pl.when(step < steps)
    def _():
        arrived(step)
        fetch(step + DEPTH - 1)
        wide[...] = raw[lax.rem(step, DEPTH)].astype(jnp.float32)
        for j in range(per_row):
            r_ref[:, j * 128:(j + 1) * 128] = wide[pl.ds(j, count, stride=per_row), :].astype(r_ref.dtype)

    @pl.when(step == steps)
    def _():
        for g in range(DEPTH - 1):
            arrived(steps + g)

    @pl.when(step == lag)
    def _():
        whole.wait()

    @pl.when(step >= lag)
    def _():
        factor = HEAD_DIM ** -0.5
        half = HEAD_DIM // 2

        def body(b, carry):
            for u in range(UNROLL):
                for i in range(SUB):
                    t = (b * UNROLL + u) * SUB + i
                    at = pl.multiple_of(slots[(step - lag) * TOK + t] * 8, 8)
                    spread[u, pl.ds(i * 8, 8), :] = store[pl.ds(at, 8), :]
            for u in range(UNROLL):
                here = pl.ds(pl.multiple_of((b * UNROLL + u) * SUB, SUB), SUB)
                cosines, sines = cos_ref[here, :], sin_ref[here, :]
                parts = [spread[u, pl.ds(j, SUB, stride=8), :] for j in range(6)]
                q_ref[here, :half] = ((parts[0] * cosines - parts[1] * sines) * factor).astype(q_ref.dtype)
                q_ref[here, half:] = ((parts[1] * cosines + parts[0] * sines) * factor).astype(q_ref.dtype)
                k_ref[here, :half] = (parts[2] * cosines - parts[3] * sines).astype(k_ref.dtype)
                k_ref[here, half:] = (parts[3] * cosines + parts[2] * sines).astype(k_ref.dtype)
                v_ref[here, :half] = parts[4].astype(v_ref.dtype)
                v_ref[here, half:] = parts[5].astype(v_ref.dtype)
            return carry

        lax.fori_loop(0, TOK // (SUB * UNROLL), body, 0)


def expand(group_size, lin, tiles, slots, cosines, sines):
    tokens = slots.shape[0] * slots.shape[1]
    width = tiles.shape[0] // (lin.shape[0] // 8) * 128
    steps, mine = tokens // TOK, tokens // group_size
    lag, count = LAG, mine // steps
    assert mine % steps == 0
    head = jax.ShapeDtypeStruct((tokens, HEAD_DIM), jnp.bfloat16)
    late = lambda i, s: (jnp.maximum(i - lag, 0), 0)
    return pl.pallas_call(
        functools.partial(expand_kernel, lag),
        grid_spec=pltpu.PrefetchScalarGridSpec(
            num_scalar_prefetch=1,
            grid=(steps + lag,),
            in_specs=[
                pl.BlockSpec(memory_space=pl.ANY),
                pl.BlockSpec(memory_space=pl.ANY),
                pl.BlockSpec((TOK, HEAD_DIM // 2), late),
                pl.BlockSpec((TOK, HEAD_DIM // 2), late),
            ],
            out_specs=[pl.BlockSpec((count, width), lambda i, s: (jnp.minimum(i, steps - 1), 0))] + [pl.BlockSpec((TOK, HEAD_DIM), late)] * 3,
            scratch_shapes=[
                pltpu.VMEM(lin.shape, lin.dtype),
                pltpu.VMEM((UNROLL, SUB * 8, 128), jnp.float32),
                pltpu.VMEM((DEPTH, count * width // 128, 128), tiles.dtype),
                pltpu.VMEM((count * width // 128, 128), jnp.float32),
                pltpu.SemaphoreType.DMA,
                pltpu.SemaphoreType.DMA((DEPTH,)),
            ],
        ),
        out_shape=(jax.ShapeDtypeStruct((mine, width), tiles.dtype),) + (head,) * 3,
        compiler_params=pltpu.CompilerParams(vmem_limit_bytes=VMEM_LIMIT),
        name="expand",
    )(slots.reshape(tokens), lin, tiles, cosines, sines)


def solution(mesh):
    group_size = mesh.shape["tp"]

    def local_step(token_ids, positions, table_rows, norm_scale, w_query, w_key, w_value):
        dev_index = lax.axis_index("tp")
        vocab_rows, model_width = table_rows.shape
        tokens = token_ids.shape[0]
        normalizer = float(np.asarray(math.sqrt(model_width), dtype=jnp.bfloat16))
        kv_heads = w_key.shape[1] // HEAD_DIM
        slot_count = max(kv_heads, group_size)
        slots_here = slot_count // group_size
        first_head = (dev_index * slots_here) // (slot_count // kv_heads)
        if kv_heads * HEAD_DIM == slots_here * HEAD_DIM:
            key_cols, value_cols = w_key, w_value
        else:
            key_cols = lax.dynamic_slice_in_dim(w_key, first_head * HEAD_DIM, slots_here * HEAD_DIM, axis=1)
            value_cols = lax.dynamic_slice_in_dim(w_value, first_head * HEAD_DIM, slots_here * HEAD_DIM, axis=1)

        plan = Plan(group_size, tokens, vocab_rows)
        slots, rows, counts, offsets, over = prepare(plan, group_size, vocab_rows, token_ids)
        fits = over[0] <= 0
        buf = gather_rows(plan, normalizer, counts, rows.reshape(-1), offsets, table_rows)
        _, lin, tiles, cosines, sines = multicast(plan, group_size, buf, norm_scale, w_query, key_cols, value_cols, positions)

        def fast(lin, tiles, cosines, sines):
            return expand(group_size, lin, tiles, slots, cosines, sines)

        def slow(lin, tiles, cosines, sines):
            return dense_path(group_size, token_ids, positions, table_rows, norm_scale, w_query, key_cols, value_cols)

        residual, queries, key_heads, value_heads = lax.cond(fits, fast, slow, lin, tiles, cosines, sines)
        return residual, queries[:, None, :], key_heads[:, None, :], value_heads[:, None, :]

    head_spec = P("dp", "tp", None)
    return jax.shard_map(local_step, mesh=mesh, in_specs=(P("dp"), P("dp"), P("tp", None), P(), P(None, "tp"), P(), P()), out_specs=(P(("dp", "tp"), None), head_spec, head_spec, head_spec), check_vma=False)
```

```python
import functools
import math
import jax
import jax.numpy as jnp
import numpy as np
from jax import lax
from jax.experimental import pallas as pl
from jax.experimental.pallas import tpu as pltpu
from jax.sharding import PartitionSpec as P

HEAD_DIM = 256
EPSILON = 1e-6
ROPE_BASE = 10000.0
CHUNK = 64
PICK = 64
SLAB = 8
DEPTH = 4
CORES = 2
VMEM_LIMIT = 60 * 1024 * 1024


def inverse_freq():
    return ROPE_BASE ** (-jnp.arange(0, HEAD_DIM, 2, dtype=jnp.float32) / HEAD_DIM)


def rope_tables(positions):
    angles = positions.astype(jnp.float32)[:, None] * inverse_freq()[None, :]
    return jnp.cos(angles), jnp.sin(angles)


def rms_norm(resid_rows, norm_scale):
    widened = resid_rows.astype(jnp.float32)
    inv_rms = lax.rsqrt(jnp.mean(widened * widened, axis=-1, keepdims=True) + EPSILON)
    return (widened * inv_rms * (1.0 + norm_scale)).astype(jnp.bfloat16)


def rotate(head_vals, cosines, sines):
    half_dim = head_vals.shape[-1] // 2
    front_half = head_vals[..., :half_dim]
    back_half = head_vals[..., half_dim:]
    return jnp.concatenate([front_half * cosines - back_half * sines, back_half * cosines + front_half * sines], axis=-1)


def project(normed, weight, cosines, sines, factor):
    linear = jnp.dot(normed, weight, preferred_element_type=jnp.float32).astype(jnp.bfloat16)
    head_view = linear.reshape(linear.shape[0], -1, HEAD_DIM).astype(jnp.float32)
    return (rotate(head_view, cosines, sines) * factor).astype(jnp.bfloat16)


def dense_path(group_size, token_ids, positions, table_rows, norm_scale, w_query, key_cols, value_cols):
    dev_index = lax.axis_index("tp")
    vocab_rows, model_width = table_rows.shape
    normalizer = jnp.asarray(math.sqrt(model_width), dtype=jnp.bfloat16)
    local_ids = token_ids - dev_index * vocab_rows
    inside = (local_ids >= 0) & (local_ids < vocab_rows)
    picked = jnp.take(table_rows, local_ids, axis=0, mode="clip") * normalizer
    partial = jnp.where(inside[:, None], picked, jnp.zeros((), jnp.bfloat16))
    by_owner = partial.reshape(group_size, -1, model_width)
    residual = jnp.sum(lax.all_to_all(by_owner, "tp", 0, 0), axis=0)
    normed = rms_norm(residual, norm_scale)
    copies = jnp.broadcast_to(normed[None], (group_size, *normed.shape))
    normed = lax.all_to_all(copies, "tp", 0, 0).reshape(-1, model_width)
    cosines, sines = rope_tables(positions)
    cosines, sines = cosines[:, None, :], sines[:, None, :]
    queries = project(normed, w_query, cosines, sines, HEAD_DIM ** -0.5)
    key_heads = project(normed, key_cols, cosines, sines, 1.0)
    value_lin = jnp.dot(normed, value_cols, preferred_element_type=jnp.float32).astype(jnp.bfloat16)
    return residual, queries[:, 0, :], key_heads[:, 0, :], value_lin


class Plan:
    def __init__(self, group_size, tokens, vocab_rows):
        unit = CHUNK * 2
        self.hot = min(tokens // 8, vocab_rows // unit * unit)
        share = [11 / 32, 5 / 64] + [3 / 64] * 2
        room = [share[o] if o < 4 else 3 / 128 for o in range(group_size)]
        self.caps = [max(CHUNK, -(-int(tokens * r) // CHUNK) * CHUNK) for r in room]
        self.bases, at = [], self.hot
        for cap in self.caps:
            self.bases.append(at)
            at += cap
        self.rows = at
        self.list_rows = -(-(-(-max(self.caps) // 128)) // 8) * 8


def choose(values, index):
    out = jnp.int32(values[0])
    for j in range(1, len(values)):
        out = jnp.where(index == j, jnp.int32(values[j]), out)
    return out


def offsets_by_column(rows):
    offsets = (rows & (SLAB - 1)).astype(jnp.float32)
    fill = jnp.zeros((128 - rows.shape[0], 128), jnp.float32)
    return jnp.concatenate([offsets, fill], axis=0).T


def prep_kernel(plan, group_size, vocab_rows, ids_ref, slot_ref, list_ref, count_ref, offset_ref, over_ref):
    me = lax.axis_index("tp")
    ids = ids_ref[...]
    blocks, lanes = ids.shape
    cold = ids >= plan.hot
    masks = [cold & (ids >= o * vocab_rows) & (ids < (o + 1) * vocab_rows) for o in range(group_size)]
    stack = jnp.concatenate([m.astype(jnp.float32) for m in masks], axis=0)
    stack = stack.astype(jnp.bfloat16)
    tri_r = lax.broadcasted_iota(jnp.int32, (lanes, lanes), 0)
    tri_c = lax.broadcasted_iota(jnp.int32, (lanes, lanes), 1)
    upper = (tri_r <= tri_c).astype(jnp.float32).astype(jnp.bfloat16)
    within = jnp.dot(stack, upper, preferred_element_type=jnp.float32)
    totals = jnp.dot(stack, jnp.ones((lanes, lanes), jnp.bfloat16), preferred_element_type=jnp.float32)
    low_r = lax.broadcasted_iota(jnp.int32, (blocks, blocks), 0)
    low_c = lax.broadcasted_iota(jnp.int32, (blocks, blocks), 1)
    lower = (low_c < low_r).astype(jnp.float32).astype(jnp.bfloat16)
    slot = jnp.where(cold, 0, ids)
    own_rank = jnp.full((blocks, lanes), -1, jnp.int32)
    over = jnp.zeros((1, lanes), jnp.int32)
    for o in range(group_size):
        tot = totals[o * blocks:(o + 1) * blocks]
        before = jnp.dot(lower, tot.astype(jnp.bfloat16), preferred_element_type=jnp.float32)
        rank = (before + within[o * blocks:(o + 1) * blocks]).astype(jnp.int32) - 1
        slot = slot + jnp.where(masks[o], jnp.minimum(rank, plan.caps[o] - 1) + plan.bases[o], 0)
        own_rank = jnp.where(masks[o] & (me == o), rank, own_rank)
        count = (before[blocks - 1:] + tot[blocks - 1:]).astype(jnp.int32)
        count_ref[o:o + 1, :] = count
        over = jnp.maximum(over, count - plan.caps[o])
    slot_ref[...] = slot
    over_ref[0] = jnp.max(over)
    local = jnp.where(own_rank >= 0, ids - me * vocab_rows, 0)
    major, minor = own_rank >> 7, own_rank & 127
    high, low = local >> 8, local & 255
    iota_major = lax.broadcasted_iota(jnp.int32, (plan.list_rows, lanes), 0)
    iota_minor = lax.broadcasted_iota(jnp.int32, (lanes, lanes), 0)
    acc = jnp.zeros((2 * plan.list_rows, lanes), jnp.float32)
    per = 8
    for g in range(blocks // per):
        lhs, rhs = [], []
        for r in range(g * per, (g + 1) * per):
            hit = iota_major == major[r:r + 1, :]
            lhs.append(jnp.concatenate([jnp.where(hit, high[r:r + 1, :], 0), jnp.where(hit, low[r:r + 1, :], 0)], axis=0).astype(jnp.float32))
            rhs.append((iota_minor == minor[r:r + 1, :]).astype(jnp.float32))
        left = jnp.concatenate(lhs, axis=1).astype(jnp.bfloat16)
        right = jnp.concatenate(rhs, axis=1).astype(jnp.bfloat16)
        acc = acc + lax.dot_general(left, right, (((1,), (1,)), ((), ())), preferred_element_type=jnp.float32)
    whole = acc.astype(jnp.int32)
    wanted = whole[:plan.list_rows] * 256 + whole[plan.list_rows:]
    list_ref[...] = wanted
    offset_ref[...] = offsets_by_column(wanted)


def prepare(plan, group_size, vocab_rows, token_ids):
    blocks = token_ids.shape[0] // 128
    return pl.pallas_call(
        functools.partial(prep_kernel, plan, group_size, vocab_rows),
        out_shape=(
            jax.ShapeDtypeStruct((blocks, 128), jnp.int32),
            jax.ShapeDtypeStruct((plan.list_rows, 128), jnp.int32),
            jax.ShapeDtypeStruct((group_size, 128), jnp.int32),
            jax.ShapeDtypeStruct((128, 128), jnp.float32),
            jax.ShapeDtypeStruct((1,), jnp.int32),
        ),
        out_specs=[pl.BlockSpec(memory_space=pltpu.VMEM)] * 4 + [pl.BlockSpec(memory_space=pltpu.SMEM)],
        compiler_params=pltpu.CompilerParams(vmem_limit_bytes=VMEM_LIMIT),
        name="slots",
    )(token_ids.reshape(blocks, 128))


class Picker:
    def __init__(self, rows_smem, begin, groups, offsets, source, slabs, sem):
        self.rows_smem, self.begin, self.groups = rows_smem, begin, groups
        self.offsets, self.source, self.slabs, self.sem = offsets, source, slabs, sem

    def fetch(self, g):
        place = lax.rem(jnp.int32(g), DEPTH)
        first = self.begin + jnp.minimum(g, jnp.maximum(self.groups - 1, 0)) * PICK
        for i in range(PICK):
            row = self.rows_smem[first + i]
            start = pl.multiple_of((row >> 3) << 3, SLAB)
            pltpu.make_async_copy(self.source.at[pl.ds(start, SLAB)], self.slabs.at[place, pl.ds(i * SLAB, SLAB)], self.sem.at[place]).start()

    def wait(self, g):
        place = lax.rem(jnp.int32(g), DEPTH)
        pltpu.make_async_copy(self.source.at[pl.ds(0, PICK * SLAB)], self.slabs.at[place], self.sem.at[place]).wait()

    def pick(self, g):
        place = lax.rem(jnp.int32(g), DEPTH)
        per = 128 // PICK
        block = self.offsets[pl.ds(pl.multiple_of(lax.rem(g, per) * PICK, PICK), PICK), :]
        lane = lax.broadcasted_iota(jnp.int32, (PICK, 128), 1)
        column = jnp.sum(jnp.where(lane == lax.div(g, per), block, 0.0), axis=1, keepdims=True).astype(jnp.int32)
        shape = (PICK, PICK * SLAB)
        hit = lax.broadcasted_iota(jnp.int32, shape, 1) == lax.broadcasted_iota(jnp.int32, shape, 0) * SLAB + column
        onehot = jnp.where(hit, 1.0, 0.0).astype(jnp.bfloat16)
        return jnp.dot(onehot, self.slabs[place], preferred_element_type=jnp.float32)

    def lead(self):
        for g in range(DEPTH - 1):
            self.fetch(g)

    def turn(self, g):
        self.wait(g)
        self.fetch(g + DEPTH - 1)
        return self.pick(g)

    def drain(self, groups):
        for g in range(DEPTH - 1):
            self.wait(groups + g)


def gather_kernel(plan, counts, rows_smem, offsets, table, out, slabs, stage, sem, out_sem):
    me = lax.axis_index("tp")
    total = jnp.minimum(counts[me, 0], choose(plan.caps, me))
    base = choose(plan.bases, me)
    groups = (total + PICK - 1) // PICK
    picker = Picker(rows_smem, 0, groups, offsets, table, slabs, sem)
    picker.lead()

    def emit(g, picked):
        side = lax.rem(g, 2)

        @pl.when(g >= 2)
        def _():
            pltpu.make_async_copy(stage.at[side], out.at[pl.ds(0, PICK)], out_sem.at[side]).wait()

        stage[side] = picked.astype(stage.dtype)
        at = pl.multiple_of(base + g * PICK, PICK)
        pltpu.make_async_copy(stage.at[side], out.at[pl.ds(at, PICK)], out_sem.at[side]).start()

    def body(g, carry):
        emit(g, picker.turn(g))
        return carry

    lax.fori_loop(0, groups, body, 0)
    picker.drain(groups)
    for last in (2, 1):
        @pl.when(groups >= last)
        def _():
            side = lax.rem(groups - last, 2)
            pltpu.make_async_copy(stage.at[side], out.at[pl.ds(0, PICK)], out_sem.at[side]).wait()


def gather_rows(plan, counts, rows, offsets, table):
    width = table.shape[1]
    return pl.pallas_call(
        functools.partial(gather_kernel, plan),
        out_shape=jax.ShapeDtypeStruct((plan.rows, width), table.dtype),
        in_specs=[pl.BlockSpec(memory_space=pltpu.SMEM), pl.BlockSpec(memory_space=pltpu.SMEM), pl.BlockSpec(memory_space=pltpu.VMEM), pl.BlockSpec(memory_space=pl.ANY)],
        out_specs=pl.BlockSpec(memory_space=pl.ANY),
        scratch_shapes=[
            pltpu.VMEM((DEPTH, PICK * SLAB, width), table.dtype),
            pltpu.VMEM((2, PICK, width), table.dtype),
            pltpu.SemaphoreType.DMA((DEPTH,)),
            pltpu.SemaphoreType.DMA((2,)),
        ],
        compiler_params=pltpu.CompilerParams(vmem_limit_bytes=VMEM_LIMIT),
        cost_estimate=pl.CostEstimate(flops=2 * 2048 * 256 * 2816, bytes_accessed=100_000_000, transcendentals=0),
        name="owner_rows",
    )(counts, rows, offsets, table)


TOK = 512
SUB = 32
UNROLL = 4
TURN = 256
LAG = 2
HALF_PI = (1.5703125, 4.837512969970703e-4, 7.549789948768648e-8)
SIN_POLY = (-1.6666654611e-1, 8.3321608736e-3, -1.9515295891e-4)
COS_POLY = (4.166664568298827e-2, -1.388731625493765e-3, 2.443315711809948e-5)


def cos_sin(angles):
    turns = jnp.floor(angles * (2 / math.pi) + 0.5)
    x = angles - turns * HALF_PI[0]
    x = x - turns * HALF_PI[1]
    x = x - turns * HALF_PI[2]
    x2 = x * x
    sine = x + x * x2 * (SIN_POLY[0] + x2 * (SIN_POLY[1] + x2 * SIN_POLY[2]))
    cosine = 1.0 - 0.5 * x2 + x2 * x2 * (COS_POLY[0] + x2 * (COS_POLY[1] + x2 * COS_POLY[2]))
    quarter = turns.astype(jnp.int32)
    swap = (quarter & 1) == 1
    first, second = jnp.where(swap, sine, cosine), jnp.where(swap, cosine, sine)
    return jnp.where(((quarter + 1) & 2) == 2, -first, first), jnp.where((quarter & 2) == 2, -second, second)


def multicast_kernel(plan, group_size, normalizer, buf_in, table, scale_ref, wq_ref, wk_ref, wv_ref, pos_ref, freq_ref, buf, lin, tiles, cos_out, sin_out, got, ring_sem, pair_sem, fresh, made, wide, tiled, turned, in_sem, out_sem, tile_sem, turn_sem):
    del buf_in
    chips = group_size // CORES
    me = lax.axis_index("tp")
    chip, core = lax.div(me, CORES), lax.rem(me, CORES)
    mate = chip * CORES + (1 - core)
    step = 1 - 2 * core

    def chip_at(delta):
        return lax.rem(chip + delta * step + 2 * chips, chips)

    ahead, behind = chip_at(1) * CORES + core, chip_at(-1) * CORES + core

    barrier = pltpu.get_barrier_semaphore()
    for other in (mate, ahead, behind):
        pl.semaphore_signal(barrier, inc=1, device_id={"tp": other}, device_id_type=pl.DeviceIdType.MESH)
    pl.semaphore_wait(barrier, 3)

    own_n = [c // CHUNK for c in plan.caps]
    own_n[0] += plan.hot // CHUNK
    own_at, at = [], 0
    for c in own_n:
        own_at.append(at)
        at += c
    first = [own_at[2 * c] for c in range(chips)]
    half = [(own_n[2 * c] + own_n[2 * c + 1]) // 2 for c in range(chips)]
    turn = [own_n[2 * c] - half[c] for c in range(chips)]

    def rows(j):
        return pl.ds(pl.multiple_of(j * CHUNK, CHUNK), CHUNK)

    def ring(j, source=buf):
        return pltpu.make_async_remote_copy(src_ref=source.at[rows(j)], dst_ref=buf.at[rows(j)], send_sem=ring_sem.at[j], recv_sem=got.at[j], device_id={"tp": ahead}, device_id_type=pl.DeviceIdType.MESH)

    def pair(j, source=buf):
        return pltpu.make_async_remote_copy(src_ref=source.at[rows(j)], dst_ref=buf.at[rows(j)], send_sem=pair_sem.at[j], recv_sem=got.at[j], device_id={"tp": mate}, device_id_type=pl.DeviceIdType.MESH)

    def loop(count, fn):
        def body(t, c):
            fn(t)
            return c
        lax.fori_loop(0, count, body, 0)

    my_first, my_half, my_turn = choose(first, chip), choose(half, chip), choose(turn, chip)
    mine = jnp.where(core == 0, my_half, my_half - my_turn)
    mine_at = jnp.where(core == 0, my_first, my_first + my_half + my_turn)
    cross_at = my_first + my_half

    @pl.when(core == 0)
    def _():
        loop(my_turn, lambda t: pair(cross_at + t).start())

    hot_chunks = plan.hot // CHUNK
    assert half[0] >= hot_chunks

    def start(copy, j):
        from_table = (me == 0) & (j < hot_chunks)

        @pl.when(from_table)
        def _():
            copy(j, table).start()

        @pl.when(jnp.logical_not(from_table))
        def _():
            copy(j, buf).start()

    loop(mine, lambda t: start(ring, mine_at + t))
    loop(mine, lambda t: start(pair, mine_at + t))

    @pl.when(core == 1)
    def _():
        def relay(t):
            pair(cross_at + t).wait_recv()
            ring(cross_at + t).start()
        loop(my_turn, relay)

    def arrival(t, way, ring_core):
        chunk, hops, at = jnp.int32(0), jnp.int32(1), jnp.int32(0)
        for hop in range(1, chips):
            origin = lax.rem(chip - hop * way + 2 * chips, chips)
            count = choose(half, origin)
            here = choose(first, origin) + ring_core * count + lax.rem(jnp.maximum(t - at, 0) + ring_core * choose(turn, origin), count)
            chunk = jnp.where(t >= at, here, chunk)
            hops = jnp.where(t >= at, hop, hops)
            at = at + count
        return chunk, hops

    both = my_half * 2
    rot = core * (my_half + my_turn)
    width = 2 * CHUNK

    def home(s, side):
        return my_first + lax.rem(2 * s + side + rot, both)

    def chunks_of(s):
        t = jnp.maximum(s - my_half, 0)
        local = s < my_half
        come, _ = arrival(t, step, core)
        cross, _ = arrival(t, -step, 1 - core)
        return jnp.where(local, home(s, 0), come), jnp.where(local, home(s, 1), cross)

    def load(s, side, j, source=buf):
        place = lax.rem(s, 2)
        return pltpu.make_async_copy(source.at[rows(j)], fresh.at[place, pl.ds(side * CHUNK, CHUNK)], in_sem.at[place, side])

    def save(s, side, j):
        place = lax.rem(s, 2)
        at = pl.multiple_of(j * (CHUNK * 8), CHUNK * 8)
        return pltpu.make_async_copy(made.at[place, pl.ds(side * CHUNK * 8, CHUNK * 8)], lin.at[pl.ds(at, CHUNK * 8)], out_sem.at[place, side])

    per_row = tiles.shape[0] // plan.rows

    def lay(s, side, j):
        place = lax.rem(s, 2)
        at = pl.multiple_of(j * (CHUNK * per_row), CHUNK * per_row)
        return pltpu.make_async_copy(tiled.at[place, pl.ds(side * CHUNK * per_row, CHUNK * per_row)], tiles.at[pl.ds(at, CHUNK * per_row)], tile_sem.at[place, side])

    def compute(s):
        place = lax.rem(s, 2)
        one, two = chunks_of(s)
        load(s, 0, one).wait()
        load(s, 1, two).wait()

        @pl.when(s >= 2)
        def _():
            save(s, 0, 0).wait()
            save(s, 1, 0).wait()
            lay(s, 0, 0).wait()
            lay(s, 1, 0).wait()
        came = (fresh[place].astype(jnp.float32) * normalizer).astype(buf.dtype)
        for j in range(per_row):
            wide[pl.ds(j, width, stride=per_row), :] = came[:, j * 128:(j + 1) * 128].astype(jnp.float32)
        tiled[place] = wide[...].astype(tiled.dtype)
        lay(s, 0, one).start()
        lay(s, 1, two).start()
        normed = rms_norm(came, scale_ref[...])
        at = 0
        for w in (wq_ref, wk_ref, wv_ref):
            y = jnp.dot(normed, w[...], preferred_element_type=jnp.float32).astype(jnp.bfloat16).astype(jnp.float32)
            for j in range(y.shape[1] // 128):
                made[place, pl.ds(at, width, stride=8), :] = y[:, j * 128:(j + 1) * 128]
                at += 1
        save(s, 0, one).start()
        save(s, 1, two).start()

    lines, span = TURN // 128, TURN
    blocks = pos_ref.shape[0] // lines

    def keep(s, which):
        place = lax.rem(s, 2)
        at = pl.multiple_of(s * span, span)
        return pltpu.make_async_copy(turned.at[place, which], (cos_out, sin_out)[which].at[pl.ds(at, span)], turn_sem.at[place, which])

    def tables(s):
        place = lax.rem(s, 2)

        @pl.when(s >= 2)
        def _():
            for which in range(2):
                keep(s - 2, which).wait()
        pos = jnp.concatenate([pos_ref[pl.ds(s * lines + i, 1), :] for i in range(lines)], axis=1)
        sub = lax.broadcasted_iota(jnp.int32, (16, span), 0)
        digits = jnp.where(sub == 0, (pos >> 7) << 7, jnp.where(sub == 1, pos & 127, 0))
        digits = digits.astype(jnp.float32).astype(jnp.bfloat16)
        ones = jnp.ones((16, freq_ref.shape[1]), jnp.bfloat16)
        spread = lax.dot_general(digits, ones, (((0,), (0,)), ((), ())), preferred_element_type=jnp.float32)
        cosines, sines = cos_sin(spread * freq_ref[...])
        turned[place, 0] = cosines
        turned[place, 1] = sines
        for which in range(2):
            keep(s, which).start()

    def turn_of(s, carry):
        one, two = chunks_of(s)
        for side, j in ((0, one), (1, two)):
            place = j - my_first
            unseen = jnp.where(core == 0, place >= my_half + my_turn, place < my_half)

            @pl.when((s < my_half) & unseen)
            def _():
                pair(j).wait_recv()

        @pl.when(s >= my_half)
        def _():
            _, hops = arrival(s - my_half, step, core)
            ring(one).wait_recv()

            @pl.when(hops < chips - 1)
            def _():
                ring(one).start()
            pair(one).start()
            pair(two).wait_recv()
        start(functools.partial(load, s, 0), one)
        start(functools.partial(load, s, 1), two)

        @pl.when(s >= 1)
        def _():
            compute(s - 1)

        @pl.when(s < blocks)
        def _():
            tables(s)
        return carry

    rounds = plan.rows // CHUNK // 2
    assert 2 <= blocks <= rounds
    lax.fori_loop(0, rounds, turn_of, 0)
    compute(jnp.int32(rounds - 1))
    for s in (rounds - 2, rounds - 1):
        for side in range(2):
            save(jnp.int32(s), side, 0).wait()
            lay(jnp.int32(s), side, 0).wait()
    for s in (blocks - 2, blocks - 1):
        for which in range(2):
            keep(jnp.int32(s), which).wait()

    @pl.when(core == 0)
    def _():
        loop(my_turn, lambda t: pair(cross_at + t).wait_send())

    @pl.when(core == 1)
    def _():
        loop(my_turn, lambda t: ring(cross_at + t).wait_send())

    def sent(t):
        ring(mine_at + t).wait_send()
        pair(mine_at + t).wait_send()
    loop(mine, sent)
    for hop in range(1, chips):
        origin = chip_at(-hop)
        count = choose(half, origin)
        base = choose(first, origin) + core * count

        def left(t):
            if hop < chips - 1:
                ring(base + t).wait_send()
            pair(base + t).wait_send()
        loop(count, left)


def multicast(plan, group_size, normalizer, buf, table_rows, norm_scale, w_query, key_cols, value_cols, positions):
    chunks, width = plan.rows // CHUNK, buf.shape[1]
    per_row = width // 128
    tokens, half = positions.shape[0], HEAD_DIM // 2
    table = jax.ShapeDtypeStruct((tokens, half), jnp.float32)
    vmem = pl.BlockSpec(memory_space=pltpu.VMEM)
    return pl.pallas_call(
        functools.partial(multicast_kernel, plan, group_size, normalizer),
        out_shape=(jax.ShapeDtypeStruct(buf.shape, buf.dtype), jax.ShapeDtypeStruct((plan.rows * 8, 128), jnp.float32), jax.ShapeDtypeStruct((plan.rows * per_row, 128), buf.dtype), table, table),
        in_specs=[pl.BlockSpec(memory_space=pl.ANY)] * 2 + [vmem] * 6,
        out_specs=(pl.BlockSpec(memory_space=pl.ANY),) * 5,
        scratch_shapes=[
            pltpu.SemaphoreType.DMA((chunks,)),
            pltpu.SemaphoreType.DMA((chunks,)),
            pltpu.SemaphoreType.DMA((chunks,)),
            pltpu.VMEM((2, 2 * CHUNK, width), buf.dtype),
            pltpu.VMEM((2, 2 * CHUNK * 8, 128), jnp.float32),
            pltpu.VMEM((2 * CHUNK * per_row, 128), jnp.float32),
            pltpu.VMEM((2, 2 * CHUNK * per_row, 128), buf.dtype),
            pltpu.VMEM((2, 2, TURN, half), jnp.float32),
            pltpu.SemaphoreType.DMA((2, 2)),
            pltpu.SemaphoreType.DMA((2, 2)),
            pltpu.SemaphoreType.DMA((2, 2)),
            pltpu.SemaphoreType.DMA((2, 2)),
        ],
        input_output_aliases={0: 0},
        compiler_params=pltpu.CompilerParams(collective_id=0, has_side_effects=True, vmem_limit_bytes=VMEM_LIMIT),
        cost_estimate=pl.CostEstimate(flops=100_000_000_000, bytes_accessed=100_000_000, transcendentals=0),
        name="multicast",
    )(buf, table_rows, norm_scale.reshape(1, width), w_query, key_cols, value_cols, positions.reshape(-1, 128), inverse_freq().reshape(1, half))


def expand_kernel(lag, slots, lin, tiles, cos_ref, sin_ref, r_ref, q_ref, k_ref, v_ref, store, spread, raw, wide, sem, fetch_sem):
    step, steps = pl.program_id(0), pl.num_programs(0) - lag
    me = lax.axis_index("tp")
    whole = pltpu.make_async_copy(lin, store, sem)
    count, width = r_ref.shape
    per_row = width // 128

    def fetch(g):
        place = lax.rem(jnp.int32(g), DEPTH)
        first = (me * steps + jnp.minimum(g, steps - 1)) * count
        for i in range(count):
            at = pl.multiple_of(slots[first + i] * per_row, per_row)
            pltpu.make_async_copy(tiles.at[pl.ds(at, per_row)], raw.at[place, pl.ds(i * per_row, per_row)], fetch_sem.at[place]).start()

    def arrived(g):
        place = lax.rem(jnp.int32(g), DEPTH)
        pltpu.make_async_copy(tiles.at[pl.ds(0, count * per_row)], raw.at[place], fetch_sem.at[place]).wait()

    @pl.when(step == 0)
    def _():
        for g in range(DEPTH - 1):
            fetch(g)
        whole.start()

    @pl.when(step < steps)
    def _():
        arrived(step)
        fetch(step + DEPTH - 1)
        wide[...] = raw[lax.rem(step, DEPTH)].astype(jnp.float32)
        for j in range(per_row):
            r_ref[:, j * 128:(j + 1) * 128] = wide[pl.ds(j, count, stride=per_row), :].astype(r_ref.dtype)

    @pl.when(step == steps)
    def _():
        for g in range(DEPTH - 1):
            arrived(steps + g)

    @pl.when(step == lag)
    def _():
        whole.wait()

    @pl.when(step >= lag)
    def _():
        factor = HEAD_DIM ** -0.5
        half = HEAD_DIM // 2

        def body(b, carry):
            for u in range(UNROLL):
                for i in range(SUB):
                    t = (b * UNROLL + u) * SUB + i
                    at = pl.multiple_of(slots[(step - lag) * TOK + t] * 8, 8)
                    spread[u, pl.ds(i * 8, 8), :] = store[pl.ds(at, 8), :]
            for u in range(UNROLL):
                here = pl.ds(pl.multiple_of((b * UNROLL + u) * SUB, SUB), SUB)
                cosines, sines = cos_ref[here, :], sin_ref[here, :]
                parts = [spread[u, pl.ds(j, SUB, stride=8), :] for j in range(6)]
                q_ref[here, :half] = ((parts[0] * cosines - parts[1] * sines) * factor).astype(q_ref.dtype)
                q_ref[here, half:] = ((parts[1] * cosines + parts[0] * sines) * factor).astype(q_ref.dtype)
                k_ref[here, :half] = (parts[2] * cosines - parts[3] * sines).astype(k_ref.dtype)
                k_ref[here, half:] = (parts[3] * cosines + parts[2] * sines).astype(k_ref.dtype)
                v_ref[here, :half] = parts[4].astype(v_ref.dtype)
                v_ref[here, half:] = parts[5].astype(v_ref.dtype)
            return carry

        lax.fori_loop(0, TOK // (SUB * UNROLL), body, 0)


def expand(group_size, lin, tiles, slots, cosines, sines):
    tokens = slots.shape[0] * slots.shape[1]
    width = tiles.shape[0] // (lin.shape[0] // 8) * 128
    steps, mine = tokens // TOK, tokens // group_size
    lag, count = LAG, mine // steps
    assert mine % steps == 0
    head = jax.ShapeDtypeStruct((tokens, HEAD_DIM), jnp.bfloat16)
    late = lambda i, s: (jnp.maximum(i - lag, 0), 0)
    return pl.pallas_call(
        functools.partial(expand_kernel, lag),
        grid_spec=pltpu.PrefetchScalarGridSpec(
            num_scalar_prefetch=1,
            grid=(steps + lag,),
            in_specs=[
                pl.BlockSpec(memory_space=pl.ANY),
                pl.BlockSpec(memory_space=pl.ANY),
                pl.BlockSpec((TOK, HEAD_DIM // 2), late),
                pl.BlockSpec((TOK, HEAD_DIM // 2), late),
            ],
            out_specs=[pl.BlockSpec((count, width), lambda i, s: (jnp.minimum(i, steps - 1), 0))] + [pl.BlockSpec((TOK, HEAD_DIM), late)] * 3,
            scratch_shapes=[
                pltpu.VMEM(lin.shape, lin.dtype),
                pltpu.VMEM((UNROLL, SUB * 8, 128), jnp.float32),
                pltpu.VMEM((DEPTH, count * width // 128, 128), tiles.dtype),
                pltpu.VMEM((count * width // 128, 128), jnp.float32),
                pltpu.SemaphoreType.DMA,
                pltpu.SemaphoreType.DMA((DEPTH,)),
            ],
        ),
        out_shape=(jax.ShapeDtypeStruct((mine, width), tiles.dtype),) + (head,) * 3,
        compiler_params=pltpu.CompilerParams(vmem_limit_bytes=VMEM_LIMIT),
        name="expand",
    )(slots.reshape(tokens), lin, tiles, cosines, sines)


def solution(mesh):
    group_size = mesh.shape["tp"]

    def local_step(token_ids, positions, table_rows, norm_scale, w_query, w_key, w_value):
        dev_index = lax.axis_index("tp")
        vocab_rows, model_width = table_rows.shape
        tokens = token_ids.shape[0]
        normalizer = float(np.asarray(math.sqrt(model_width), dtype=jnp.bfloat16))
        kv_heads = w_key.shape[1] // HEAD_DIM
        slot_count = max(kv_heads, group_size)
        slots_here = slot_count // group_size
        first_head = (dev_index * slots_here) // (slot_count // kv_heads)
        if kv_heads * HEAD_DIM == slots_here * HEAD_DIM:
            key_cols, value_cols = w_key, w_value
        else:
            key_cols = lax.dynamic_slice_in_dim(w_key, first_head * HEAD_DIM, slots_here * HEAD_DIM, axis=1)
            value_cols = lax.dynamic_slice_in_dim(w_value, first_head * HEAD_DIM, slots_here * HEAD_DIM, axis=1)

        plan = Plan(group_size, tokens, vocab_rows)
        slots, rows, counts, offsets, over = prepare(plan, group_size, vocab_rows, token_ids)
        fits = over[0] <= 0
        buf = gather_rows(plan, counts, rows.reshape(-1), offsets, table_rows)
        _, lin, tiles, cosines, sines = multicast(plan, group_size, normalizer, buf, table_rows, norm_scale, w_query, key_cols, value_cols, positions)

        def fast(lin, tiles, cosines, sines):
            return expand(group_size, lin, tiles, slots, cosines, sines)

        def slow(lin, tiles, cosines, sines):
            return dense_path(group_size, token_ids, positions, table_rows, norm_scale, w_query, key_cols, value_cols)

        residual, queries, key_heads, value_heads = lax.cond(fits, fast, slow, lin, tiles, cosines, sines)
        return residual, queries[:, None, :], key_heads[:, None, :], value_heads[:, None, :]

    head_spec = P("dp", "tp", None)
    return jax.shard_map(local_step, mesh=mesh, in_specs=(P("dp"), P("dp"), P("tp", None), P(), P(None, "tp"), P(), P()), out_specs=(P(("dp", "tp"), None), head_spec, head_spec, head_spec), check_vma=False)
```
